8 devices in a mesh: sys: 2 (over z, y), row: 4 (over x, core).
Axes of the slice: x: 2, y: 2, z: 1, core: 2. Of those that a mesh axis runs over, the one named last changes fastest.
Arguments:
- positions: bfloat16 [16384, 768], P(('sys', 'row')), parts along dimension 0
- charges: float32 [16384], P(('sys', 'row')), parts along dimension 0
- counts: int32 [8], P(('sys', 'row')), parts along dimension 0
Outputs:
- output 1: float32 [16384, 768], P(('sys', 'row')), parts along dimension 0
- output 2: float32 [2], P('sys'), parts along dimension 0
There are 2 independent parts. The reference program is written for one: setup_inputs(seed, part) draws one part's arguments, and reference() takes and returns one part's arrays. A program takes and returns all parts, laid end to end along the dimension named above; each array names one.
All inputs are finite; a program needn't handle non-finite values.
Results may differ from the reference program's by a relative error of at most 0.001.
Values are sent between devices in bfloat16 or wider.
A program may use at most 1 GiB of HBM per device.

```python
import jax
import jax.numpy as jnp
from jax import lax

BLOCK_ROWS = 2048
D = 768
RING_SIZE = 4
NUM_ROWS = RING_SIZE * BLOCK_ROWS
ROW_TILE = min(BLOCK_ROWS, 256)


def setup_inputs(seed: int = 0, part: int = 0) -> dict:
    part_key = jax.random.fold_in(jax.random.key(seed), part)
    sub_keys = jax.random.split(part_key, 6)
    positions = jax.random.normal(sub_keys[0], (NUM_ROWS, D), jnp.float32).astype(jnp.bfloat16)
    sign_vals = jnp.where(jax.random.bernoulli(sub_keys[1], 0.5, (NUM_ROWS,)), 1.0, -1.0)
    magnitude = jax.random.uniform(sub_keys[2], (NUM_ROWS,), jnp.float32, 0.5, 1.5)
    charges = (sign_vals * magnitude).astype(jnp.float32)
    counts = jax.random.randint(sub_keys[3], (RING_SIZE,), BLOCK_ROWS // 16, BLOCK_ROWS + 1)
    full_slot = jax.random.randint(sub_keys[4], (), 0, RING_SIZE)
    small_slot = (full_slot + jax.random.randint(sub_keys[5], (), 1, RING_SIZE)) % RING_SIZE
    counts = counts.at[full_slot].set(BLOCK_ROWS).at[small_slot].set(BLOCK_ROWS // 16)
    return {'positions': positions, 'charges': charges, 'counts': counts.astype(jnp.int32)}


def reference(positions, charges, counts):
    is_valid = jnp.arange(BLOCK_ROWS)[None, :] < counts[:, None]
    live_q = jnp.where(is_valid, charges.reshape(RING_SIZE, BLOCK_ROWS), 0.0).reshape(NUM_ROWS)
    pos_f32 = positions.astype(jnp.float32)
    sq_norm = jnp.sum(pos_f32 * pos_f32, axis=1)
    col_ids = jnp.arange(NUM_ROWS)
    neg_scale = -0.5 / D
    inv_len2 = 1.0 / D

    def tile_terms(tile_idx):
        row_start = tile_idx * ROW_TILE
        row_block = lax.dynamic_slice(positions, (row_start, 0), (ROW_TILE, D))
        row_q = lax.dynamic_slice(live_q, (row_start,), (ROW_TILE,))
        row_sq = lax.dynamic_slice(sq_norm, (row_start,), (ROW_TILE,))
        gram_mat = jnp.dot(row_block, positions.T, preferred_element_type=jnp.float32)
        dist_sq = jnp.maximum(row_sq[:, None] + sq_norm[None, :] - 2.0 * gram_mat, 0.0)
        weight = row_q[:, None] * live_q[None, :] * jnp.exp(dist_sq * neg_scale)
        row_ids = row_start + jnp.arange(ROW_TILE)
        weight = jnp.where(row_ids[:, None] == col_ids[None, :], 0.0, weight)
        pulled = jnp.dot(weight.astype(jnp.bfloat16), positions, preferred_element_type=jnp.float32)
        row_force = (jnp.sum(weight, axis=1)[:, None] * row_block.astype(jnp.float32) - pulled) * inv_len2
        return row_force, jnp.sum(weight)

    tile_forces, tile_energy = lax.map(tile_terms, jnp.arange(NUM_ROWS // ROW_TILE))
    return tile_forces.reshape(NUM_ROWS, D), (0.5 * jnp.sum(tile_energy)).reshape(1)
```

```python
import functools

import jax
import jax.numpy as jnp
from jax import lax
from jax.experimental import pallas as pl
from jax.experimental.pallas import tpu as pltpu
from jax.sharding import PartitionSpec as P


CHUNK = 128
ROW_TILE = 1024
COL_CHUNKS = 4
COL_TILE = CHUNK * COL_CHUNKS
LOG2E = 1.4426950408889634
F32 = jnp.float32


def exchange_kernel(mine_ref, all_ref, local_sem, send_sems, recv_sems):
    me = lax.axis_index('row')
    n = all_ref.shape[0]
    barrier = pltpu.get_barrier_semaphore()
    for d in range(1, n):
        pl.semaphore_signal(barrier, inc=1, device_id={'row': lax.rem(me + d, n)}, device_id_type=pl.DeviceIdType.MESH)
    pl.semaphore_wait(barrier, n - 1)
    local = pltpu.make_async_copy(mine_ref, all_ref.at[me], local_sem)
    local.start()
    sends = []
    for d in range(1, n):
        copy = pltpu.make_async_remote_copy(
            src_ref=mine_ref, dst_ref=all_ref.at[me], send_sem=send_sems.at[d - 1], recv_sem=recv_sems.at[d - 1],
            device_id={'row': lax.rem(me + d, n)}, device_id_type=pl.DeviceIdType.MESH)
        copy.start()
        sends.append(copy)
    for d in range(1, n):
        src = lax.rem(me + n - d, n)
        pltpu.make_async_remote_copy(
            src_ref=mine_ref, dst_ref=all_ref.at[src], send_sem=send_sems.at[d - 1], recv_sem=recv_sems.at[d - 1],
            device_id={'row': src}, device_id_type=pl.DeviceIdType.MESH).wait_recv()
    for copy in sends:
        copy.wait_send()
    local.wait()


def exchange(mine, n, collective_id):
    vmem = pl.BlockSpec(memory_space=pltpu.VMEM)
    return pl.pallas_call(
        exchange_kernel,
        out_shape=jax.ShapeDtypeStruct((n,) + mine.shape, mine.dtype),
        in_specs=[vmem], out_specs=vmem,
        scratch_shapes=[pltpu.SemaphoreType.DMA, pltpu.SemaphoreType.DMA((n - 1,)), pltpu.SemaphoreType.DMA((n - 1,))],
        compiler_params=pltpu.CompilerParams(collective_id=collective_id, has_side_effects=True),
        name='exchange%d' % collective_id,
    )(mine)


def step_kernel(cfg, *refs):
    sources, first, last, diag, kappa, inv_len2 = cfg
    refs = list(refs)
    scal, x_hbm, rowf_hbm, tab_hbm = refs[:4]
    refs = refs[4:]
    src_hbm = [] if diag else refs[:len(sources)]
    refs = refs[len(src_hbm):]
    if not first:
        t_in, s_in = refs[:2]
        refs = refs[2:]
    out_a, out_b = refs[:2]
    xv, rowv, tabv, xc, tv, sv, lids, in_sems, col_sem, t_sems, out_sems = refs[2:]
    rows, width = xv.shape
    num_rt = rows // ROW_TILE
    me = scal[4]
    live_rt = (scal[me] + ROW_TILE - 1) // ROW_TILE

    fetch = [pltpu.make_async_copy(x_hbm, xv, in_sems.at[0]), pltpu.make_async_copy(rowf_hbm, rowv, in_sems.at[1]),
             pltpu.make_async_copy(tab_hbm, tabv, in_sems.at[2])]
    for copy in fetch:
        copy.start()

    def t_copies(rt):
        sl = pl.ds(rt * ROW_TILE, ROW_TILE)
        return (pltpu.make_async_copy(t_in.at[sl], tv.at[sl], t_sems.at[2 * rt]),
                pltpu.make_async_copy(s_in.at[sl], sv.at[sl], t_sems.at[2 * rt + 1]))

    if not first:
        for rt in range(num_rt):
            @pl.when(rt < live_rt)
            def _():
                for copy in t_copies(rt):
                    copy.start()

    count = jnp.int32(0)
    if diag:
        cols = xv
        count = (scal[me] + CHUNK - 1) // CHUNK
    else:
        cols = xc
        for k, (xor, start, num) in enumerate(sources):
            block = me ^ xor
            live = jnp.clip((scal[block] + CHUNK - 1) // CHUNK - start, 0, num)

            def put(j, _, k=k, base=count, tag=block * (rows // CHUNK) + start):
                pltpu.make_async_copy(src_hbm[k].at[pl.ds(pl.multiple_of(j * CHUNK, CHUNK), CHUNK)],
                                      xc.at[pl.ds(pl.multiple_of((base + j) * CHUNK, CHUNK), CHUNK)], col_sem).start()
                lids[base + j] = tag + j
                return 0
            lax.fori_loop(0, live, put, 0)
            count = count + live
    tiles = (count + COL_CHUNKS - 1) // COL_CHUNKS
    if not diag:
        zero_id = tab_hbm.shape[0] // 2 - 1

        def pad(j, _):
            pltpu.make_async_copy(x_hbm.at[pl.ds(0, CHUNK)], xc.at[pl.ds(pl.multiple_of(j * CHUNK, CHUNK), CHUNK)], col_sem).start()
            lids[j] = zero_id
            return 0
        lax.fori_loop(count, tiles * COL_CHUNKS, pad, 0)

        def drain(j, _):
            pltpu.make_async_copy(x_hbm.at[pl.ds(0, CHUNK)], xc.at[pl.ds(0, CHUNK)], col_sem).wait()
            return 0
        lax.fori_loop(0, tiles * COL_CHUNKS, drain, 0)
    for copy in fetch:
        copy.wait()
    half_tab = tab_hbm.shape[0] // 2

    def tile(rt, ct):
        r0 = pl.multiple_of(rt * ROW_TILE, ROW_TILE)
        c0 = pl.multiple_of(ct * COL_TILE, COL_TILE)
        rsl = pl.ds(r0, ROW_TILE)
        s_sum = sv[rsl, :]
        row_a = rowv[0, rsl, :]
        row_c = rowv[1, rsl, :]
        parts = []
        for q in range(COL_CHUNKS // 2):
            gram = lax.dot_general(xv[rsl, :], cols[pl.ds(c0 + q * 256, 256), :], (((1,), (1,)), ((), ())),
                                   preferred_element_type=F32)
            for h in range(2):
                k = 2 * q + h
                if diag:
                    cid = me * (rows // CHUNK) + ct * COL_CHUNKS + k
                else:
                    cid = lids[ct * COL_CHUNKS + k]
                col_a = tabv[pl.ds(cid, 1), :]
                col_c = tabv[pl.ds(half_tab + cid, 1), :]
                expo = jnp.minimum(gram[:, h * 128:(h + 1) * 128] * (2.0 * kappa) + row_a + col_a, 0.0)
                w = jnp.exp2(expo) * (row_c * col_c)
                if diag:
                    delta = (lax.broadcasted_iota(jnp.int32, w.shape, 0) - lax.broadcasted_iota(jnp.int32, w.shape, 1))
                    w = jnp.where(delta == c0 + k * CHUNK - r0, 0.0, w)
                s_sum = s_sum + w
                parts.append(w.astype(jnp.bfloat16))
        sv[rsl, :] = s_sum
        w_all = jnp.concatenate(parts, axis=1)
        tv[rsl, :] += jnp.dot(w_all, cols[pl.ds(c0, COL_TILE), :], preferred_element_type=F32)

    def out_copies(rt):
        sl = pl.ds(rt * ROW_TILE, ROW_TILE)
        if last:
            return (pltpu.make_async_copy(tv.at[sl], out_a.at[sl], out_sems.at[2 * rt]),)
        return (pltpu.make_async_copy(tv.at[sl], out_a.at[sl], out_sems.at[2 * rt]),
                pltpu.make_async_copy(sv.at[sl], out_b.at[sl], out_sems.at[2 * rt + 1]))

    if last:
        out_b[...] = jnp.zeros_like(out_b)
    if first:
        def clear(i, _):
            sl = pl.ds(pl.multiple_of(i * 64, 64), 64)
            tv[sl, :] = jnp.zeros((64, width), F32)
            sv[sl, :] = jnp.zeros((64, 128), F32)
            return 0
        lax.fori_loop(0, rows // 64, clear, 0)

    def row_tile(rt, _):
        if not first:
            r0 = pl.multiple_of(rt * ROW_TILE, ROW_TILE)
            sl = pl.ds(r0, ROW_TILE)
            pltpu.make_async_copy(t_in.at[sl], tv.at[sl], t_sems.at[2 * rt]).wait()
            pltpu.make_async_copy(s_in.at[sl], sv.at[sl], t_sems.at[2 * rt + 1]).wait()

        def one(ct, _):
            tile(rt, ct)
            return 0
        lax.fori_loop(0, tiles, one, 0)
        if last:
            def finish(i, acc):
                sl = pl.ds(pl.multiple_of(rt * ROW_TILE + i * 64, 64), 64)
                total = jnp.sum(sv[sl, :], axis=1, keepdims=True)
                tv[sl, :] = (total * xv[sl, :].astype(F32) - tv[sl, :]) * inv_len2
                part = sv[pl.ds(pl.multiple_of(rt * ROW_TILE + i * 64, 64), 8), :]
                for g in range(1, 8):
                    part = part + sv[pl.ds(pl.multiple_of(rt * ROW_TILE + i * 64 + g * 8, 8), 8), :]
                return acc + part
            out_b[...] += lax.fori_loop(0, ROW_TILE // 64, finish, jnp.zeros((8, 128), F32))
        sl = pl.ds(pl.multiple_of(rt * ROW_TILE, ROW_TILE), ROW_TILE)
        pltpu.make_async_copy(tv.at[sl], out_a.at[sl], out_sems.at[2 * rt]).start()
        if not last:
            pltpu.make_async_copy(sv.at[sl], out_b.at[sl], out_sems.at[2 * rt + 1]).start()
        return 0
    lax.fori_loop(0, live_rt, row_tile, 0)

    for rt in range(num_rt):
        if last:
            @pl.when(rt >= live_rt)
            def _():
                sl = pl.ds(rt * ROW_TILE, ROW_TILE)
                tv[sl, :] = jnp.zeros((ROW_TILE, width), F32)
                out_copies(rt)[0].start()
            out_copies(rt)[0].wait()
        else:
            @pl.when(rt < live_rt)
            def _():
                for copy in out_copies(rt):
                    copy.wait()


def step(scal, x, rowf, tab, srcs, sources, carry, last, diag):
    rows, width = x.shape
    first = carry is None
    cfg = (sources, first, last, diag, LOG2E * 0.5 / width, 1.0 / width)
    ins = [scal, x, rowf, tab] + ([] if diag else list(srcs)) + ([] if first else list(carry))
    hbm = pl.BlockSpec(memory_space=pl.ANY)
    in_specs = [pl.BlockSpec(memory_space=pltpu.SMEM)] + [hbm] * (len(ins) - 1)
    if last:
        out_shape = (jax.ShapeDtypeStruct((rows, width), F32), jax.ShapeDtypeStruct((8, 128), F32))
        out_specs = (hbm, pl.BlockSpec(memory_space=pltpu.VMEM))
        alias = {}
    else:
        out_shape = (jax.ShapeDtypeStruct((rows, width), F32), jax.ShapeDtypeStruct((rows, 128), F32))
        out_specs = (hbm, hbm)
        alias = {} if first else {len(ins) - 2: 0, len(ins) - 1: 1}
    max_chunks = sum(num for _, _, num in sources)
    max_chunks = -(-max_chunks // COL_CHUNKS) * COL_CHUNKS
    num_rt = rows // ROW_TILE
    flops = int(4 * rows * max_chunks * CHUNK * width * 0.6)
    return pl.pallas_call(
        functools.partial(step_kernel, cfg),
        out_shape=out_shape, in_specs=in_specs, out_specs=out_specs,
        scratch_shapes=[
            pltpu.VMEM((rows, width), jnp.bfloat16),
            pltpu.VMEM((2, rows, 128), F32),
            pltpu.VMEM(tab.shape, F32),
            pltpu.VMEM((CHUNK if diag else max_chunks * CHUNK, width), jnp.bfloat16),
            pltpu.VMEM((rows, width), F32),
            pltpu.VMEM((rows, 128), F32),
            pltpu.SMEM((max_chunks,), jnp.int32),
            pltpu.SemaphoreType.DMA((3,)),
            pltpu.SemaphoreType.DMA,
            pltpu.SemaphoreType.DMA((2 * num_rt,)),
            pltpu.SemaphoreType.DMA((2 * num_rt,)),
        ],
        input_output_aliases=alias,
        compiler_params=pltpu.CompilerParams(vmem_limit_bytes=60 * 1024 * 1024),
        cost_estimate=pl.CostEstimate(flops=flops, bytes_accessed=rows * width * 10, transcendentals=0),
        name='step_%s' % ('own' if diag else 'last' if last else 'mid'),
    )(*ins)


PIECES = (512, 512, 512, 256, 256)


def solution(mesh):
    num_blocks = mesh.shape['row']
    cross_perm = [(src, src ^ 2) for src in range(num_blocks)]
    pair_perm = [(src, src ^ 1) for src in range(num_blocks)]

    def per_device(positions, charges, counts):
        rows, width = positions.shape
        me = lax.axis_index('row')
        kappa = LOG2E * 0.5 / width
        pieces, off = [], 0
        for size in PIECES:
            pieces.append((off, lax.ppermute(positions[off:off + size], 'row', cross_perm)))
            off += size
        partner = lax.ppermute(positions, 'row', pair_perm)
        pos_f32 = positions.astype(F32)
        row_a = -kappa * jnp.sum(pos_f32 * pos_f32, axis=1)
        live_q = jnp.where(jnp.arange(rows) < counts[0], charges, 0.0)
        chunks = rows // CHUNK
        mine = jnp.concatenate([row_a.reshape(chunks, CHUNK), live_q.reshape(chunks, CHUNK),
                                jnp.broadcast_to(counts.astype(F32)[0], (8, CHUNK))], axis=0)
        rowf = jnp.stack([jnp.broadcast_to(row_a[:, None], (rows, 128)), jnp.broadcast_to(live_q[:, None], (rows, 128))])
        every = exchange(mine, num_blocks, 1)
        pad = jnp.zeros((8, CHUNK), F32)
        tab = jnp.concatenate([every[:, :chunks].reshape(-1, CHUNK), pad, every[:, chunks:2 * chunks].reshape(-1, CHUNK), pad], axis=0)
        scal = jnp.concatenate([every[:, 2 * chunks, 0].astype(jnp.int32), me.reshape(1).astype(jnp.int32)])

        carry = step(scal, positions, rowf, tab, (), ((0, 0, chunks),), None, False, True)
        carry = step(scal, positions, rowf, tab, (partner,), ((1, 0, chunks),), carry, False, False)
        for k, (off, piece) in enumerate(pieces):
            relay = lax.ppermute(piece, 'row', pair_perm)
            num = PIECES[k] // CHUNK
            carry = step(scal, positions, rowf, tab, (piece, relay), ((2, off // CHUNK, num), (3, off // CHUNK, num)), carry,
                         k == len(pieces) - 1, False)
        forces, part = carry
        parts = exchange(part, num_blocks, 2)
        return forces, 0.5 * jnp.sum(parts).reshape(1)

    row_spec = P(('sys', 'row'), None)
    vec_spec = P(('sys', 'row'))
    return jax.shard_map(per_device, mesh=mesh, in_specs=(row_spec, vec_spec, vec_spec), out_specs=(row_spec, P('sys')), check_vma=False)
```

```python
import functools

import jax
import jax.numpy as jnp
from jax import lax
from jax.experimental import pallas as pl
from jax.experimental.pallas import tpu as pltpu
from jax.sharding import PartitionSpec as P


CHUNK = 128
ROW_TILE = 1024
LOG2E = 1.4426950408889634
F32 = jnp.float32
MESH = pl.DeviceIdType.MESH
VMEM_SPEC = pl.BlockSpec(memory_space=pltpu.VMEM)
HBM_SPEC = pl.BlockSpec(memory_space=pl.ANY)


def to_all(mine_ref, all_ref, local_sem, send_sems, recv_sems):
    me = lax.axis_index('row')
    n = all_ref.shape[0]
    barrier = pltpu.get_barrier_semaphore()
    for d in range(1, n):
        pl.semaphore_signal(barrier, inc=1, device_id={'row': lax.rem(me + d, n)}, device_id_type=MESH)
    pl.semaphore_wait(barrier, n - 1)
    local = pltpu.make_async_copy(mine_ref, all_ref.at[me], local_sem)
    local.start()
    sends = []
    for d in range(1, n):
        copy = pltpu.make_async_remote_copy(
            src_ref=mine_ref, dst_ref=all_ref.at[me], send_sem=send_sems.at[d - 1], recv_sem=recv_sems.at[d - 1],
            device_id={'row': lax.rem(me + d, n)}, device_id_type=MESH)
        copy.start()
        sends.append(copy)
    for d in range(1, n):
        src = lax.rem(me + n - d, n)
        pltpu.make_async_remote_copy(
            src_ref=mine_ref, dst_ref=all_ref.at[src], send_sem=send_sems.at[d - 1], recv_sem=recv_sems.at[d - 1],
            device_id={'row': src}, device_id_type=MESH).wait_recv()
    for copy in sends:
        copy.wait_send()
    local.wait()


def sems(n):
    return [pltpu.SemaphoreType.DMA, pltpu.SemaphoreType.DMA((n - 1,)), pltpu.SemaphoreType.DMA((n - 1,))]


def energy_kernel(mine_ref, out_ref, all_ref, local_sem, send_sems, recv_sems):
    to_all(mine_ref, all_ref, local_sem, send_sems, recv_sems)
    total = all_ref[0]
    for k in range(1, all_ref.shape[0]):
        total = total + all_ref[k]
    total = jnp.sum(total, axis=1, keepdims=True)
    out_ref[...] = 0.5 * jnp.sum(total, axis=0, keepdims=True)


def energy_call(mine, n):
    return pl.pallas_call(
        energy_kernel,
        out_shape=jax.ShapeDtypeStruct((1, 1), F32),
        in_specs=[VMEM_SPEC], out_specs=VMEM_SPEC,
        scratch_shapes=[pltpu.VMEM((n,) + mine.shape, mine.dtype)] + sems(n),
        compiler_params=pltpu.CompilerParams(collective_id=2, has_side_effects=True),
        name='energy',
    )(mine)


def count_of(info_ref):
    return jnp.max(info_ref[info_ref.shape[0] - 8:, :]).astype(jnp.int32)


def step_kernel(cfg, *refs):
    start, num, tile_chunks, first, last, diag, kappa, inv_len2 = cfg
    refs = list(refs)
    xv, rowv, my_info = refs[:3]
    refs = refs[3:]
    cols, src_info = xv, my_info
    if not diag:
        src_info, cols = refs[:2]
        refs = refs[2:]
    if not first:
        t_in, s_in = refs[:2]
        refs = refs[2:]
    if last:
        forces, part, out_sems = refs
        tv, sv = t_in, s_in
    else:
        tv, sv = refs
    rows, width = xv.shape
    block_chunks = rows // CHUNK
    num_rt = rows // ROW_TILE
    col_tile = tile_chunks * CHUNK
    live_rt = (count_of(my_info) + ROW_TILE - 1) // ROW_TILE
    live = jnp.clip((count_of(src_info) + CHUNK - 1) // CHUNK - start, 0, num)
    tiles = (live + tile_chunks - 1) // tile_chunks

    def tile(rt, ct):
        r0 = pl.multiple_of(rt * ROW_TILE, ROW_TILE)
        c0 = pl.multiple_of(ct * col_tile, col_tile)
        rsl = pl.ds(r0, ROW_TILE)
        s_sum = sv[rsl, :]
        row_a = rowv[0, rsl, :]
        row_c = rowv[1, rsl, :]
        parts = []
        for q in range(tile_chunks // 2):
            gram = lax.dot_general(xv[rsl, :], cols[pl.ds(c0 + q * 256, 256), :], (((1,), (1,)), ((), ())),
                                   preferred_element_type=F32)
            for h in range(2):
                k = 2 * q + h
                cid = start + ct * tile_chunks + k
                col_a = src_info[pl.ds(cid, 1), :]
                col_c = src_info[pl.ds(block_chunks + cid, 1), :]
                expo = jnp.minimum(gram[:, h * 128:(h + 1) * 128] * (2.0 * kappa) + row_a + col_a, 0.0)
                w = jnp.exp2(expo) * (row_c * col_c)
                if diag:
                    delta = lax.broadcasted_iota(jnp.int32, w.shape, 0) - lax.broadcasted_iota(jnp.int32, w.shape, 1)
                    w = jnp.where(delta == c0 + k * CHUNK - r0, 0.0, w)
                s_sum = s_sum + w
                parts.append(w.astype(jnp.bfloat16))
        sv[rsl, :] = s_sum
        w_all = jnp.concatenate(parts, axis=1)
        tv[rsl, :] += jnp.dot(w_all, cols[pl.ds(c0, col_tile), :], preferred_element_type=F32)

    if first:
        def clear(i, _):
            sl = pl.ds(pl.multiple_of(i * 64, 64), 64)
            tv[sl, :] = jnp.zeros((64, width), F32)
            sv[sl, :] = jnp.zeros((64, 128), F32)
            return 0

        lax.fori_loop(0, rows // 64, clear, 0)
    if last:
        part[...] = jnp.zeros_like(part)

    def row_tile(rt, _):
        def one(ct, _):
            tile(rt, ct)
            return 0

        lax.fori_loop(0, tiles, one, 0)
        if last:
            def finish(i, acc):
                base = rt * ROW_TILE + i * 64
                sl = pl.ds(pl.multiple_of(base, 64), 64)
                sums = sv[sl, :]
                total = jnp.sum(sums, axis=1, keepdims=True)
                tv[sl, :] = (total * xv[sl, :].astype(F32) - tv[sl, :]) * inv_len2
                for g in range(8):
                    acc = acc + sums[g * 8:(g + 1) * 8]
                return acc

            part[...] += lax.fori_loop(0, ROW_TILE // 64, finish, jnp.zeros((8, 128), F32))
            sl = pl.ds(pl.multiple_of(rt * ROW_TILE, ROW_TILE), ROW_TILE)
            pltpu.make_async_copy(tv.at[sl], forces.at[sl], out_sems.at[rt]).start()
        return 0

    lax.fori_loop(0, live_rt, row_tile, 0)

    if last:
        for rt in range(num_rt):
            sl = pl.ds(rt * ROW_TILE, ROW_TILE)

            @pl.when(rt >= live_rt)
            def _():
                tv[sl, :] = jnp.zeros((ROW_TILE, width), F32)
                pltpu.make_async_copy(tv.at[sl], forces.at[sl], out_sems.at[rt]).start()
        for rt in range(num_rt):
            sl = pl.ds(rt * ROW_TILE, ROW_TILE)
            pltpu.make_async_copy(tv.at[sl], forces.at[sl], out_sems.at[rt]).wait()


VMEM_LIMIT = 24 * 1024 * 1024


def step(x, rowf, my_info, src_info, cols, start, num, tile_chunks, carry, last):
    rows, width = x.shape
    first, diag = carry is None, cols is None
    cfg = (start, num, tile_chunks, first, last, diag, LOG2E * 0.5 / width, 1.0 / width)
    ins = [x, rowf, my_info] + ([] if diag else [src_info, cols]) + ([] if first else list(carry))
    in_specs = [VMEM_SPEC] * len(ins)
    num_rt = rows // ROW_TILE
    flops = int(4 * rows * num * CHUNK * width * 0.6)
    common = dict(
        in_specs=in_specs,
        compiler_params=pltpu.CompilerParams(vmem_limit_bytes=VMEM_LIMIT),
        cost_estimate=pl.CostEstimate(flops=flops, bytes_accessed=rows * width, transcendentals=0),
        name='step_%d_%d' % (start, num))
    kernel = functools.partial(step_kernel, cfg)
    if last:
        return pl.pallas_call(
            kernel,
            out_shape=(jax.ShapeDtypeStruct((rows, width), F32), jax.ShapeDtypeStruct((8, 128), F32)),
            out_specs=(HBM_SPEC, VMEM_SPEC),
            scratch_shapes=[pltpu.SemaphoreType.DMA((num_rt,))], **common)(*ins)
    return pl.pallas_call(
        kernel,
        out_shape=(pltpu.VMEM((rows, width), F32), pltpu.VMEM((rows, 128), F32)),
        out_specs=(VMEM_SPEC, VMEM_SPEC),
        input_output_aliases={} if first else {len(ins) - 2: 0, len(ins) - 1: 1}, **common)(*ins)


PIECES = (256, 512, 512, 512, 256)


def after(value, *others):
    return lax.optimization_barrier((value,) + others)[0]


def solution(mesh):
    num_blocks = mesh.shape['row']
    cross_perm = [(src, src ^ 2) for src in range(num_blocks)]
    pair_perm = [(src, src ^ 1) for src in range(num_blocks)]

    def per_device(positions, charges, counts):
        rows, width = positions.shape
        chunks = rows // CHUNK
        kappa = LOG2E * 0.5 / width
        head = positions[:PIECES[0]]
        arrived = [lax.ppermute(head, 'row', cross_perm)]
        positions = after(positions, head)
        pos_f32 = positions.astype(F32)
        row_a = -kappa * jnp.sum(pos_f32 * pos_f32, axis=1)
        live_q = jnp.where(jnp.arange(rows) < counts[0], charges, 0.0)
        info = jnp.concatenate([row_a.reshape(chunks, CHUNK), live_q.reshape(chunks, CHUNK),
                                jnp.broadcast_to(counts.astype(F32)[0], (8, CHUNK))], axis=0)
        info_cross = lax.ppermute(info, 'row', cross_perm)
        info_pair = lax.ppermute(info, 'row', pair_perm)
        x = pltpu.with_memory_space_constraint(positions, pltpu.VMEM)
        off = PIECES[0]
        for size in PIECES[1:]:
            arrived.append(lax.ppermute(positions[off:off + size], 'row', cross_perm))
            off += size
        partner = lax.ppermute(positions, 'row', pair_perm)
        rowf = jnp.stack([jnp.broadcast_to(row_a[:, None], (rows, 128)), jnp.broadcast_to(live_q[:, None], (rows, 128))])
        rowf = pltpu.with_memory_space_constraint(rowf, pltpu.VMEM)

        carry = step(x, rowf, info, None, None, 0, chunks, 4, None, False)
        partner, *carry = lax.optimization_barrier((partner, *carry))
        carry = step(x, rowf, info, info_pair, partner, 0, chunks, 4, carry, False)
        info_cross, *carry = lax.optimization_barrier((info_cross, *carry))
        info_diag = lax.ppermute(info_cross, 'row', pair_perm)
        off = 0
        for k, piece in enumerate(arrived):
            num = PIECES[k] // CHUNK
            piece, *carry = lax.optimization_barrier((piece, *carry))
            relay = lax.ppermute(piece, 'row', pair_perm)
            carry = step(x, rowf, info, info_cross, piece, off, num, min(4, num), carry, False)
            carry = step(x, rowf, info, info_diag, relay, off, num, min(4, num), carry, k == len(PIECES) - 1)
            off += num
        forces, part = carry
        return forces, energy_call(part, num_blocks).reshape(1)

    row_spec = P(('sys', 'row'), None)
    vec_spec = P(('sys', 'row'))
    return jax.shard_map(per_device, mesh=mesh, in_specs=(row_spec, vec_spec, vec_spec), out_specs=(row_spec, P('sys')), check_vma=False)
```

```python
import functools

import jax
import jax.numpy as jnp
from jax import lax
from jax.experimental import pallas as pl
from jax.experimental.pallas import tpu as pltpu
from jax.sharding import PartitionSpec as P


CHUNK = 128
ROW_TILE = 1024
LOG2E = 1.4426950408889634
F32 = jnp.float32
VMEM_SPEC = pl.BlockSpec(memory_space=pltpu.VMEM)
HBM_SPEC = pl.BlockSpec(memory_space=pl.ANY)
FINISH_TILE = 128


def prep_kernel(kappa, x_hbm, q_ref, count_ref, xv, rowv, info, sems):
    rows = xv.shape[0]
    chunks = rows // CHUNK
    part = rows // 4
    for k in range(4):
        pltpu.make_async_copy(x_hbm.at[pl.ds(k * part, part)], xv.at[pl.ds(k * part, part)], sems.at[k]).start()
    eye = lax.broadcasted_iota(jnp.int32, (CHUNK, CHUNK), 0) == lax.broadcasted_iota(jnp.int32, (CHUNK, CHUNK), 1)
    lane = lax.broadcasted_iota(jnp.int32, (1, CHUNK), 1)
    count = count_ref[0]
    info[2 * chunks:, :] = jnp.full((8, CHUNK), count, jnp.int32).astype(F32)
    for k in range(4):
        pltpu.make_async_copy(x_hbm.at[pl.ds(k * part, part)], xv.at[pl.ds(k * part, part)], sems.at[k]).wait()

        def one(c, _):
            sl = pl.ds(pl.multiple_of(c * CHUNK, CHUNK), CHUNK)
            block = xv[sl, :].astype(F32)
            col_s = -kappa * jnp.sum(block * block, axis=1, keepdims=True)
            rowv[0, sl, :] = jnp.broadcast_to(col_s, (CHUNK, CHUNK))
            info[pl.ds(c, 1), :] = jnp.sum(jnp.where(eye, col_s, 0.0), axis=0, keepdims=True)
            live = jnp.where(lane + c * CHUNK < count, q_ref[pl.ds(c, 1), :], 0.0)
            info[pl.ds(chunks + c, 1), :] = live
            rowv[1, sl, :] = jnp.broadcast_to(jnp.sum(jnp.where(eye, live, 0.0), axis=1, keepdims=True), (CHUNK, CHUNK))
            return 0
        lax.fori_loop(k * chunks // 4, (k + 1) * chunks // 4, one, 0)


def prep(positions, charges, counts):
    rows, width = positions.shape
    chunks = rows // CHUNK
    return pl.pallas_call(
        functools.partial(prep_kernel, LOG2E * 0.5 / width),
        out_shape=[pltpu.VMEM((rows, width), positions.dtype), pltpu.VMEM((2, rows, CHUNK), F32),
                   jax.ShapeDtypeStruct((2 * chunks + 8, CHUNK), F32)],
        in_specs=[HBM_SPEC, VMEM_SPEC, pl.BlockSpec(memory_space=pltpu.SMEM)], out_specs=[VMEM_SPEC] * 3,
        scratch_shapes=[pltpu.SemaphoreType.DMA((4,))],
        compiler_params=pltpu.CompilerParams(vmem_limit_bytes=VMEM_LIMIT),
        name='prep')(positions, charges.reshape(chunks, CHUNK), counts)


def count_of(info_ref):
    return jnp.max(info_ref[info_ref.shape[0] - 8:, :]).astype(jnp.int32)


def step_kernel(cfg, *refs):
    start, num, tile_chunks, first, last, diag, kappa = cfg
    refs = list(refs)
    xv, rowv, my_info = refs[:3]
    refs = refs[3:]
    cols, src_info = xv, my_info
    if not diag:
        src_info, cols = refs[:2]
        refs = refs[2:]
    if not first:
        refs = refs[2:]
    tv, sv = refs[:2]
    rows, width = xv.shape
    block_chunks = rows // CHUNK
    col_tile = tile_chunks * CHUNK
    live_rt = (count_of(my_info) + ROW_TILE - 1) // ROW_TILE
    live = jnp.clip((count_of(src_info) + CHUNK - 1) // CHUNK - start, 0, num)
    tiles = (live + tile_chunks - 1) // tile_chunks

    def tile(rt, ct):
        r0 = pl.multiple_of(rt * ROW_TILE, ROW_TILE)
        c0 = pl.multiple_of(ct * col_tile, col_tile)
        rsl = pl.ds(r0, ROW_TILE)
        s_sum = sv[rsl, :]
        row_a = rowv[0, rsl, :]
        row_c = rowv[1, rsl, :]
        parts = []
        for q in range(tile_chunks // 2):
            gram = lax.dot_general(xv[rsl, :], cols[pl.ds(c0 + q * 256, 256), :], (((1,), (1,)), ((), ())),
                                   preferred_element_type=F32)
            for h in range(2):
                k = 2 * q + h
                cid = start + ct * tile_chunks + k
                col_a = src_info[pl.ds(cid, 1), :]
                col_c = src_info[pl.ds(block_chunks + cid, 1), :]
                expo = jnp.minimum(gram[:, h * 128:(h + 1) * 128] * (2.0 * kappa) + row_a + col_a, 0.0)
                w = jnp.exp2(expo) * (row_c * col_c)
                if diag:
                    delta = lax.broadcasted_iota(jnp.int32, w.shape, 0) - lax.broadcasted_iota(jnp.int32, w.shape, 1)
                    w = jnp.where(delta == c0 + k * CHUNK - r0, 0.0, w)
                s_sum = s_sum + w
                parts.append(w.astype(jnp.bfloat16))
        sv[rsl, :] = s_sum
        w_all = jnp.concatenate(parts, axis=1)
        tv[rsl, :] += jnp.dot(w_all, cols[pl.ds(c0, col_tile), :], preferred_element_type=F32)

    if first:
        def clear(i, _):
            sl = pl.ds(pl.multiple_of(i * 64, 64), 64)
            tv[sl, :] = jnp.zeros((64, width), F32)
            sv[sl, :] = jnp.zeros((64, 128), F32)
            return 0
        lax.fori_loop(0, rows // 64, clear, 0)
    def row_tile(rt, _):
        def one(ct, _):
            tile(rt, ct)
            return 0
        lax.fori_loop(0, tiles, one, 0)
        return 0
    lax.fori_loop(0, live_rt, row_tile, 0)

    if last:
        def add(i, acc):
            sums = sv[pl.ds(pl.multiple_of(i * 128, 128), 128), :]
            for g in range(16):
                acc = acc + sums[g * 8:(g + 1) * 8]
            return acc
        refs[2][...] = lax.fori_loop(0, rows // 128, add, jnp.zeros((8, 128), F32))


def finish_kernel(inv_len2, xv, tv, sv, forces, buf, out_sems):
    num = xv.shape[0] // FINISH_TILE

    def out(i):
        return pltpu.make_async_copy(
            buf.at[lax.rem(i, 4)], forces.at[pl.ds(pl.multiple_of(i * FINISH_TILE, FINISH_TILE), FINISH_TILE)], out_sems.at[lax.rem(i, 4)])

    def one(i, _):
        @pl.when(i >= 4)
        def _():
            out(i - 4).wait()
        sl = pl.ds(pl.multiple_of(i * FINISH_TILE, FINISH_TILE), FINISH_TILE)
        total = jnp.sum(sv[sl, :], axis=1, keepdims=True)
        buf[lax.rem(i, 4)] = (total * xv[sl, :].astype(F32) - tv[sl, :]) * inv_len2
        out(i).start()
        return 0
    lax.fori_loop(0, num, one, 0)
    for i in range(num - 4, num):
        out(i).wait()


def finish(x, tv, sv):
    rows, width = x.shape
    return pl.pallas_call(
        functools.partial(finish_kernel, 1.0 / width),
        out_shape=jax.ShapeDtypeStruct((rows, width), F32),
        in_specs=[VMEM_SPEC] * 3, out_specs=HBM_SPEC,
        scratch_shapes=[pltpu.VMEM((4, FINISH_TILE, width), F32), pltpu.SemaphoreType.DMA((4,))],
        compiler_params=pltpu.CompilerParams(vmem_limit_bytes=VMEM_LIMIT),
        cost_estimate=pl.CostEstimate(flops=rows * width * 1000, bytes_accessed=rows * width * 4, transcendentals=0),
        name='finish')(x, tv, sv)


VMEM_LIMIT = 24 * 1024 * 1024


def step(x, rowf, my_info, src_info, cols, start, num, tile_chunks, carry, last):
    rows, width = x.shape
    first, diag = carry is None, cols is None
    cfg = (start, num, tile_chunks, first, last, diag, LOG2E * 0.5 / width)
    ins = [x, rowf, my_info] + ([] if diag else [src_info, cols]) + ([] if first else list(carry))
    in_specs = [VMEM_SPEC] * len(ins)
    flops = int(4 * rows * num * CHUNK * width * 0.6)
    common = dict(
        in_specs=in_specs,
        compiler_params=pltpu.CompilerParams(vmem_limit_bytes=VMEM_LIMIT),
        cost_estimate=pl.CostEstimate(flops=flops, bytes_accessed=rows * width, transcendentals=0),
        name='step_%d_%d' % (start, num))
    kernel = functools.partial(step_kernel, cfg)
    part_shape = [jax.ShapeDtypeStruct((8, 128), F32)] if last else []
    return pl.pallas_call(
        kernel,
        out_shape=[pltpu.VMEM((rows, width), F32), pltpu.VMEM((rows, 128), F32)] + part_shape,
        out_specs=[VMEM_SPEC] * (2 + len(part_shape)),
        input_output_aliases={} if first else {len(ins) - 2: 0, len(ins) - 1: 1}, **common)(*ins)


PIECES = (256, 512, 512, 512, 256)


def after(value, *others):
    return lax.optimization_barrier((value,) + others)[0]


def solution(mesh):
    num_blocks = mesh.shape['row']
    cross_perm = [(src, src ^ 2) for src in range(num_blocks)]
    pair_perm = [(src, src ^ 1) for src in range(num_blocks)]
    diag_perm = [(src, src ^ 3) for src in range(num_blocks)]

    def per_device(positions, charges, counts):
        rows, _ = positions.shape
        chunks = rows // CHUNK
        head = positions[:PIECES[0]]
        arrived = [lax.ppermute(head, 'row', cross_perm)]
        positions = after(positions, head)
        x, rowf, info = prep(positions, charges, counts)
        info_cross = lax.ppermute(info, 'row', cross_perm)
        info_pair = lax.ppermute(info, 'row', pair_perm)
        off = PIECES[0]
        for size in PIECES[1:]:
            arrived.append(lax.ppermute(positions[off:off + size], 'row', cross_perm))
            off += size
        partner = lax.ppermute(positions, 'row', pair_perm)
        carry = step(x, rowf, info, None, None, 0, chunks, 4, None, False)
        partner, *carry = lax.optimization_barrier((partner, *carry))
        carry = step(x, rowf, info, info_pair, partner, 0, chunks, 4, carry, False)
        info_cross, *carry = lax.optimization_barrier((info_cross, *carry))
        info_diag = lax.ppermute(info_cross, 'row', pair_perm)
        off = 0
        for k, piece in enumerate(arrived):
            num = PIECES[k] // CHUNK
            piece, *carry = lax.optimization_barrier((piece, *carry))
            relay = lax.ppermute(piece, 'row', pair_perm)
            carry = step(x, rowf, info, info_cross, piece, off, num, min(4, num), carry, False)
            carry = step(x, rowf, info, info_diag, relay, off, num, min(4, num), carry, k == len(PIECES) - 1)
            off += num
        t_sum, s_sum, part = carry
        total = part
        for perm in (cross_perm, pair_perm, diag_perm):
            total = total + lax.ppermute(part, 'row', perm)
        forces = finish(x, t_sum, s_sum)
        return forces, (0.5 * jnp.sum(total)).reshape(1)

    row_spec = P(('sys', 'row'), None)
    vec_spec = P(('sys', 'row'))
    return jax.shard_map(per_device, mesh=mesh, in_specs=(row_spec, vec_spec, vec_spec), out_specs=(row_spec, P('sys')), check_vma=False)
```

```python
import functools

import jax
import jax.numpy as jnp
from jax import lax
from jax.experimental import pallas as pl
from jax.experimental.pallas import tpu as pltpu
from jax.sharding import PartitionSpec as P


CHUNK = 128
SUB_ROWS = 512
LOG2E = 1.4426950408889634
F32 = jnp.float32
VMEM_SPEC = pl.BlockSpec(memory_space=pltpu.VMEM)
HBM_SPEC = pl.BlockSpec(memory_space=pl.ANY)
FINISH_TILE = 256


def prep_kernel(kappa, xv, q_ref, count_ref, rowv, info):
    rows = xv.shape[0]
    chunks = rows // CHUNK
    eye = lax.broadcasted_iota(jnp.int32, (CHUNK, CHUNK), 0) == lax.broadcasted_iota(jnp.int32, (CHUNK, CHUNK), 1)
    lane = lax.broadcasted_iota(jnp.int32, (1, CHUNK), 1)
    count = count_ref[0]
    info[2 * chunks:, :] = jnp.full((8, CHUNK), count, jnp.int32).astype(F32)

    def one(c, _):
        sl = pl.ds(pl.multiple_of(c * CHUNK, CHUNK), CHUNK)
        block = xv[sl, :].astype(F32)
        col_s = -kappa * jnp.sum(block * block, axis=1, keepdims=True)
        rowv[0, sl, :] = jnp.broadcast_to(col_s, (CHUNK, CHUNK))
        info[pl.ds(c, 1), :] = jnp.sum(jnp.where(eye, col_s, 0.0), axis=0, keepdims=True)
        live = jnp.where(lane + c * CHUNK < count, q_ref[pl.ds(c, 1), :], 0.0)
        info[pl.ds(chunks + c, 1), :] = live
        rowv[1, sl, :] = jnp.broadcast_to(jnp.sum(jnp.where(eye, live, 0.0), axis=1, keepdims=True), (CHUNK, CHUNK))
        return 0

    lax.fori_loop(0, chunks, one, 0)


def prep(x, charges, counts):
    rows, width = x.shape
    chunks = rows // CHUNK
    return pl.pallas_call(
        functools.partial(prep_kernel, LOG2E * 0.5 / width),
        out_shape=[pltpu.VMEM((2, rows, CHUNK), F32),
                   jax.ShapeDtypeStruct((2 * chunks + 8, CHUNK), F32)],
        in_specs=[VMEM_SPEC, VMEM_SPEC, pl.BlockSpec(memory_space=pltpu.SMEM)], out_specs=[VMEM_SPEC] * 2,
        compiler_params=pltpu.CompilerParams(vmem_limit_bytes=VMEM_LIMIT),
        name='prep')(x, charges.reshape(chunks, CHUNK), counts)


def count_of(info_ref):
    return jnp.max(info_ref[info_ref.shape[0] - 8:, :]).astype(jnp.int32)


def weights(kappa, gram, row_a, row_c, col_a, col_c):
    expo = jnp.minimum(gram * (2.0 * kappa) + row_a + col_a, 0.0)
    return jnp.exp2(expo) * (row_c * col_c)


def step_kernel(cfg, *refs):
    start, num, tile_chunks, first, diag, kappa = cfg
    refs = list(refs)
    xv, rowv, my_info = refs[:3]
    refs = refs[3:]
    cols, src_info = xv, my_info
    if not diag:
        src_info, cols = refs[:2]
        refs = refs[2:]
    if not first:
        refs = refs[2:]
    tv, sv = refs[:2]
    rows, width = xv.shape
    block_chunks = rows // CHUNK
    col_tile = tile_chunks * CHUNK
    live = jnp.clip((count_of(src_info) + CHUNK - 1) // CHUNK - start, 0, num)
    tiles = (live + tile_chunks - 1) // tile_chunks

    def weigh(ct, c0, r0):
        rsl = pl.ds(r0, SUB_ROWS)
        s_sum = sv[rsl, :]
        row_a = rowv[0, rsl, :]
        row_c = rowv[1, rsl, :]
        parts = []
        for q in range(tile_chunks // 2):
            gram = lax.dot_general(xv[rsl, :], cols[pl.ds(c0 + q * 256, 256), :], (((1,), (1,)), ((), ())),
                                   preferred_element_type=F32)
            for h in range(2):
                k = 2 * q + h
                cid = start + ct * tile_chunks + k
                col_a = src_info[pl.ds(cid, 1), :]
                col_c = src_info[pl.ds(block_chunks + cid, 1), :]
                w = weights(kappa, gram[:, h * 128:(h + 1) * 128], row_a, row_c, col_a, col_c)
                if diag:
                    delta = lax.broadcasted_iota(jnp.int32, w.shape, 0) - lax.broadcasted_iota(jnp.int32, w.shape, 1)
                    w = jnp.where(delta == c0 + k * CHUNK - r0, 0.0, w)
                s_sum = s_sum + w
                parts.append(w.astype(jnp.bfloat16))
        sv[rsl, :] = s_sum
        return jnp.concatenate(parts, axis=1)

    def pull(w, c0, r0):
        tv[pl.ds(r0, SUB_ROWS), :] += jnp.dot(w, cols[pl.ds(c0, col_tile), :], preferred_element_type=F32)

    def tile(ct, _):
        c0 = pl.multiple_of(ct * col_tile, col_tile)
        w = None
        for r0 in range(0, rows, SUB_ROWS):
            w_next = weigh(ct, c0, r0)
            if w is not None:
                pull(w, c0, r0 - SUB_ROWS)
            w = w_next
        pull(w, c0, rows - SUB_ROWS)
        return 0

    if first:
        def clear(i, _):
            sl = pl.ds(pl.multiple_of(i * 64, 64), 64)
            tv[sl, :] = jnp.zeros((64, width), F32)
            sv[sl, :] = jnp.zeros((64, 128), F32)
            return 0

        lax.fori_loop(0, rows // 64, clear, 0)
    lax.fori_loop(0, tiles, tile, 0)


def last_kernel(cfg, *refs):
    start, num, total, kappa = cfg
    xv, rowv, src_info, cols, _, sv, wv = refs[:7]
    block_chunks = xv.shape[0] // CHUNK

    def row_tile(rt, acc):
        rsl = pl.ds(pl.multiple_of(rt * SUB_ROWS, SUB_ROWS), SUB_ROWS)
        sums = sv[rsl, :]
        gram = lax.dot_general(xv[rsl, :], cols[...], (((1,), (1,)), ((), ())), preferred_element_type=F32)
        for k in range(num):
            w = weights(kappa, gram[:, k * CHUNK:(k + 1) * CHUNK], rowv[0, rsl, :], rowv[1, rsl, :],
                        src_info[start + k:start + k + 1, :], src_info[block_chunks + start + k:block_chunks + start + k + 1, :])
            sums = sums + w
            wv[rsl, k * CHUNK:(k + 1) * CHUNK] = w.astype(jnp.bfloat16)
        sv[rsl, :] = sums
        if total:
            for g in range(SUB_ROWS // 8):
                acc = acc + sums[g * 8:(g + 1) * 8]
        return acc

    part = lax.fori_loop(0, xv.shape[0] // SUB_ROWS, row_tile, jnp.zeros((8, 128), F32))
    if total:
        refs[7][...] = part


def last_step(x, rowf, src_info, cols, start, s_sum, total):
    rows, width = x.shape
    num = cols.shape[0] // CHUNK
    ins = [x, rowf, src_info, cols, s_sum]
    part_shape = [jax.ShapeDtypeStruct((8, 128), F32)] if total else []
    return pl.pallas_call(
        functools.partial(last_kernel, (start, num, total, LOG2E * 0.5 / width)),
        out_shape=[pltpu.VMEM((rows, 128), F32), pltpu.VMEM((rows, num * CHUNK), jnp.bfloat16)] + part_shape,
        in_specs=[VMEM_SPEC] * len(ins), out_specs=[VMEM_SPEC] * (2 + len(part_shape)),
        input_output_aliases={len(ins) - 1: 0},
        compiler_params=pltpu.CompilerParams(vmem_limit_bytes=VMEM_LIMIT),
        cost_estimate=pl.CostEstimate(flops=2 * rows * num * CHUNK * width, bytes_accessed=rows * width, transcendentals=0))(*ins)


def finish_kernel(inv_len2, xv, tv, sv, wa, wb, cols_a, cols_b, forces, buf, out_sems):
    num = xv.shape[0] // FINISH_TILE

    def out(i):
        return pltpu.make_async_copy(
            buf.at[lax.rem(i, 4)], forces.at[pl.ds(pl.multiple_of(i * FINISH_TILE, FINISH_TILE), FINISH_TILE)], out_sems.at[lax.rem(i, 4)])

    def one(i, _):
        @pl.when(i >= 4)
        def _():
            out(i - 4).wait()

        sl = pl.ds(pl.multiple_of(i * FINISH_TILE, FINISH_TILE), FINISH_TILE)
        total = jnp.sum(sv[sl, :], axis=1, keepdims=True)
        pulled = (tv[sl, :] + jnp.dot(wa[sl, :], cols_a[...], preferred_element_type=F32)
                  + jnp.dot(wb[sl, :], cols_b[...], preferred_element_type=F32))
        buf[lax.rem(i, 4)] = (total * xv[sl, :].astype(F32) - pulled) * inv_len2
        out(i).start()
        return 0

    lax.fori_loop(0, num, one, 0)
    for i in range(num - 4, num):
        out(i).wait()


def finish(*ins):
    x = ins[0]
    rows, width = x.shape
    return pl.pallas_call(
        functools.partial(finish_kernel, 1.0 / width),
        out_shape=jax.ShapeDtypeStruct((rows, width), F32),
        in_specs=[VMEM_SPEC] * len(ins), out_specs=HBM_SPEC,
        scratch_shapes=[pltpu.VMEM((4, FINISH_TILE, width), F32), pltpu.SemaphoreType.DMA((4,))],
        compiler_params=pltpu.CompilerParams(vmem_limit_bytes=VMEM_LIMIT),
        cost_estimate=pl.CostEstimate(flops=rows * width * 1000, bytes_accessed=rows * width * 4, transcendentals=0),
        name='finish')(*ins)


VMEM_LIMIT = 24 * 1024 * 1024


def step(x, rowf, my_info, src_info, cols, start, num, tile_chunks, carry):
    rows, width = x.shape
    first, diag = carry is None, cols is None
    cfg = (start, num, tile_chunks, first, diag, LOG2E * 0.5 / width)
    ins = [x, rowf, my_info] + ([] if diag else [src_info, cols]) + ([] if first else list(carry))
    in_specs = [VMEM_SPEC] * len(ins)
    flops = int(4 * rows * num * CHUNK * width * 0.6)
    common = dict(
        in_specs=in_specs,
        compiler_params=pltpu.CompilerParams(vmem_limit_bytes=VMEM_LIMIT),
        cost_estimate=pl.CostEstimate(flops=flops, bytes_accessed=rows * width, transcendentals=0),
        name='step_%d_%d' % (start, num))
    kernel = functools.partial(step_kernel, cfg)
    return pl.pallas_call(
        kernel,
        out_shape=[pltpu.VMEM((rows, width), F32), pltpu.VMEM((rows, 128), F32)],
        out_specs=[VMEM_SPEC] * 2,
        input_output_aliases={} if first else {len(ins) - 2: 0, len(ins) - 1: 1}, **common)(*ins)


PIECES = (256, 512, 512, 512, 256)


def after(value, *others):
    return lax.optimization_barrier((value,) + others)[0]


def solution(mesh):
    num_blocks = mesh.shape['row']
    cross_perm = [(src, src ^ 2) for src in range(num_blocks)]
    pair_perm = [(src, src ^ 1) for src in range(num_blocks)]
    diag_perm = [(src, src ^ 3) for src in range(num_blocks)]

    def per_device(positions, charges, counts):
        rows, _ = positions.shape
        chunks = rows // CHUNK
        x = pltpu.with_memory_space_constraint(positions, pltpu.VMEM)
        head = positions[:PIECES[0]]
        arrived = [lax.ppermute(head, 'row', cross_perm)]
        positions = after(positions, head)
        rowf, info = prep(x, charges, counts)
        info_cross = lax.ppermute(info, 'row', cross_perm)
        info_pair = lax.ppermute(info, 'row', pair_perm)
        off = PIECES[0]
        for size in PIECES[1:]:
            arrived.append(lax.ppermute(positions[off:off + size], 'row', cross_perm))
            off += size
        partner = lax.ppermute(positions, 'row', pair_perm)
        carry = step(x, rowf, info, None, None, 0, chunks, 4, None)
        partner, *carry = lax.optimization_barrier((partner, *carry))
        carry = step(x, rowf, info, info_pair, partner, 0, chunks, 4, carry)
        info_cross, *carry = lax.optimization_barrier((info_cross, *carry))
        info_diag = lax.ppermute(info_cross, 'row', pair_perm)
        off = 0
        for k, piece in enumerate(arrived):
            num = PIECES[k] // CHUNK
            piece, *carry = lax.optimization_barrier((piece, *carry))
            relay = lax.ppermute(piece, 'row', pair_perm)
            if k < len(PIECES) - 1:
                carry = step(x, rowf, info, info_cross, piece, off, num, min(4, num), carry)
                carry = step(x, rowf, info, info_diag, relay, off, num, min(4, num), carry)
            else:
                t_sum, s_sum = carry
                s_sum, w_piece = last_step(x, rowf, info_cross, piece, off, s_sum, False)
                s_sum, w_relay, part = last_step(x, rowf, info_diag, relay, off, s_sum, True)
            off += num
        total = part
        for perm in (cross_perm, pair_perm, diag_perm):
            total = total + lax.ppermute(part, 'row', perm)
        forces = finish(x, t_sum, s_sum, w_piece, w_relay, piece, relay)
        return forces, (0.5 * jnp.sum(total)).reshape(1)

    row_spec = P(('sys', 'row'), None)
    vec_spec = P(('sys', 'row'))
    return jax.shard_map(per_device, mesh=mesh, in_specs=(row_spec, vec_spec, vec_spec), out_specs=(row_spec, P('sys')), check_vma=False)
```

```python
import functools

import jax
import jax.numpy as jnp
from jax import lax
from jax.experimental import pallas as pl
from jax.experimental.pallas import tpu as pltpu
from jax.sharding import PartitionSpec as P


CHUNK = 128
SUB_ROWS = 512
LOG2E = 1.4426950408889634
F32 = jnp.float32
VMEM_SPEC = pl.BlockSpec(memory_space=pltpu.VMEM)
HBM_SPEC = pl.BlockSpec(memory_space=pl.ANY)
FINISH_TILE = 256


def count_of(info_ref):
    return jnp.max(info_ref[info_ref.shape[0] - 8:, :]).astype(jnp.int32)


def live_tiles(info_ref):
    return (count_of(info_ref) + FINISH_TILE - 1) // FINISH_TILE


def prep_kernel(kappa, raw, q_ref, count_ref, xv, rowv, info, forces, zeros, sem):
    rows = raw.shape[0]
    chunks = rows // CHUNK
    eye = lax.broadcasted_iota(jnp.int32, (CHUNK, CHUNK), 0) == lax.broadcasted_iota(jnp.int32, (CHUNK, CHUNK), 1)
    lane = lax.broadcasted_iota(jnp.int32, (1, CHUNK), 1)
    count = count_ref[0]
    tiles = rows // FINISH_TILE
    live = (count + FINISH_TILE - 1) // FINISH_TILE
    zeros[...] = jnp.zeros_like(zeros)

    def blank(i):
        return pltpu.make_async_copy(zeros, forces.at[pl.ds(pl.multiple_of(i * FINISH_TILE, FINISH_TILE), FINISH_TILE)], sem)

    def start(i, _):
        blank(i).start()
        return 0

    lax.fori_loop(live, tiles, start, 0)
    info[2 * chunks:, :] = jnp.full((8, CHUNK), count, jnp.int32).astype(F32)

    def one(c, _):
        sl = pl.ds(pl.multiple_of(c * CHUNK, CHUNK), CHUNK)
        row_ids = lax.broadcasted_iota(jnp.int32, (CHUNK, 1), 0) + c * CHUNK
        block = jnp.where(row_ids < count, raw[sl, :].astype(F32), 0.0)
        xv[sl, :] = block.astype(xv.dtype)
        col_s = -kappa * jnp.sum(block * block, axis=1, keepdims=True)
        rowv[0, sl, :] = jnp.broadcast_to(col_s, (CHUNK, CHUNK))
        info[pl.ds(c, 1), :] = jnp.sum(jnp.where(eye, col_s, 0.0), axis=0, keepdims=True)
        live = jnp.where(lane + c * CHUNK < count, q_ref[pl.ds(c, 1), :], 0.0)
        info[pl.ds(chunks + c, 1), :] = live
        rowv[1, sl, :] = jnp.broadcast_to(jnp.sum(jnp.where(eye, live, 0.0), axis=1, keepdims=True), (CHUNK, CHUNK))
        return 0

    lax.fori_loop(0, chunks, one, 0)

    def wait(i, _):
        blank(i).wait()
        return 0

    lax.fori_loop(live, tiles, wait, 0)


def prep(x, charges, counts):
    rows, width = x.shape
    chunks = rows // CHUNK
    return pl.pallas_call(
        functools.partial(prep_kernel, LOG2E * 0.5 / width),
        out_shape=[jax.ShapeDtypeStruct(x.shape, x.dtype), pltpu.VMEM((2, rows, CHUNK), F32),
                   jax.ShapeDtypeStruct((2 * chunks + 8, CHUNK), F32), jax.ShapeDtypeStruct((rows, width), F32)],
        in_specs=[VMEM_SPEC, VMEM_SPEC, pl.BlockSpec(memory_space=pltpu.SMEM)], out_specs=[VMEM_SPEC] * 3 + [HBM_SPEC],
        scratch_shapes=[pltpu.VMEM((FINISH_TILE, width), F32), pltpu.SemaphoreType.DMA],
        compiler_params=pltpu.CompilerParams(vmem_limit_bytes=VMEM_LIMIT),
        name='prep')(x, charges.reshape(chunks, CHUNK), counts)


def weights(kappa, gram, row_a, row_c, col_a, col_c):
    expo = jnp.minimum(gram * (2.0 * kappa) + row_a + col_a, 0.0)
    return jnp.exp2(expo) * (row_c * col_c)


def step_kernel(cfg, *refs):
    start, num, tile_chunks, first, diag, kappa = cfg
    refs = list(refs)
    xv, rowv, my_info = refs[:3]
    refs = refs[3:]
    cols, src_info = xv, my_info
    if not diag:
        src_info, cols = refs[:2]
        refs = refs[2:]
    if not first:
        refs = refs[2:]
    tv, sv = refs[:2]
    rows, width = xv.shape
    block_chunks = rows // CHUNK
    col_tile = tile_chunks * CHUNK
    live = jnp.clip((count_of(src_info) + CHUNK - 1) // CHUNK - start, 0, num)
    tiles = (live + tile_chunks - 1) // tile_chunks

    def weigh(ct, c0, r0):
        rsl = pl.ds(r0, SUB_ROWS)
        s_sum = sv[rsl, :]
        row_a = rowv[0, rsl, :]
        row_c = rowv[1, rsl, :]
        parts = []
        for q in range(tile_chunks // 2):
            gram = lax.dot_general(xv[rsl, :], cols[pl.ds(c0 + q * 256, 256), :], (((1,), (1,)), ((), ())),
                                   preferred_element_type=F32)
            for h in range(2):
                k = 2 * q + h
                cid = start + ct * tile_chunks + k
                col_a = src_info[pl.ds(cid, 1), :]
                col_c = src_info[pl.ds(block_chunks + cid, 1), :]
                w = weights(kappa, gram[:, h * 128:(h + 1) * 128], row_a, row_c, col_a, col_c)
                if diag:
                    delta = lax.broadcasted_iota(jnp.int32, w.shape, 0) - lax.broadcasted_iota(jnp.int32, w.shape, 1)
                    w = jnp.where(delta == c0 + k * CHUNK - r0, 0.0, w)
                s_sum = s_sum + w
                parts.append(w.astype(jnp.bfloat16))
        sv[rsl, :] = s_sum
        return jnp.concatenate(parts, axis=1)

    def pull(w, c0, r0):
        tv[pl.ds(r0, SUB_ROWS), :] += jnp.dot(w, cols[pl.ds(c0, col_tile), :], preferred_element_type=F32)

    def tile(ct, _):
        c0 = pl.multiple_of(ct * col_tile, col_tile)
        w = None
        for r0 in range(0, rows, SUB_ROWS):
            w_next = weigh(ct, c0, r0)
            if w is not None:
                pull(w, c0, r0 - SUB_ROWS)
            w = w_next
        pull(w, c0, rows - SUB_ROWS)
        return 0

    if first:
        def clear(i, _):
            sl = pl.ds(pl.multiple_of(i * 64, 64), 64)
            tv[sl, :] = jnp.zeros((64, width), F32)
            sv[sl, :] = jnp.zeros((64, 128), F32)
            return 0

        lax.fori_loop(0, rows // 64, clear, 0)
    lax.fori_loop(0, tiles, tile, 0)


def pair_kernel(cfg, xv, rowv, info_a, info_b, cols_a, cols_b, t_in, s_in, tv, sv, xc):
    start, kappa = cfg
    block_chunks = xv.shape[0] // CHUNK
    xc[:CHUNK, :] = cols_a[...]
    xc[CHUNK:, :] = cols_b[...]

    @pl.when(jnp.maximum(count_of(info_a), count_of(info_b)) > start * CHUNK)
    def _():
        w_old = None
        for r0 in range(0, xv.shape[0] + SUB_ROWS, SUB_ROWS):
            w_new = None
            if r0 < xv.shape[0]:
                rsl = pl.ds(r0, SUB_ROWS)
                gram = lax.dot_general(xv[rsl, :], xc[...], (((1,), (1,)), ((), ())), preferred_element_type=F32)
                w = [weights(kappa, gram[:, k * CHUNK:(k + 1) * CHUNK], rowv[0, rsl, :], rowv[1, rsl, :],
                             info[start:start + 1, :], info[block_chunks + start:block_chunks + start + 1, :])
                     for k, info in enumerate((info_a, info_b))]
                sv[rsl, :] += w[0] + w[1]
                w_new = jnp.concatenate([part.astype(jnp.bfloat16) for part in w], axis=1)
            if w_old is not None:
                tv[pl.ds(r0 - SUB_ROWS, SUB_ROWS), :] += jnp.dot(w_old, xc[...], preferred_element_type=F32)
            w_old = w_new


def pair_step(x, rowf, infos, cols, start, carry):
    rows, width = x.shape
    ins = [x, rowf, *infos, *cols, *carry]
    return pl.pallas_call(
        functools.partial(pair_kernel, (start, LOG2E * 0.5 / width)),
        out_shape=[pltpu.VMEM((rows, width), F32), pltpu.VMEM((rows, 128), F32)],
        in_specs=[VMEM_SPEC] * len(ins), out_specs=[VMEM_SPEC] * 2,
        scratch_shapes=[pltpu.VMEM((2 * CHUNK, width), x.dtype)],
        input_output_aliases={len(ins) - 2: 0, len(ins) - 1: 1},
        compiler_params=pltpu.CompilerParams(vmem_limit_bytes=VMEM_LIMIT),
        cost_estimate=pl.CostEstimate(flops=8 * rows * CHUNK * width, bytes_accessed=rows * width, transcendentals=0))(*ins)


def last_kernel(cfg, *refs):
    start, half, kappa = cfg
    xv, rowv, src_info, cols = refs[:4]
    sv, wv = refs[6:8] if half else refs[5:7]
    block_chunks = xv.shape[0] // CHUNK

    def row_tile(rt, acc):
        rsl = pl.ds(pl.multiple_of(rt * SUB_ROWS, SUB_ROWS), SUB_ROWS)
        gram = lax.dot_general(xv[rsl, :], cols[...], (((1,), (1,)), ((), ())), preferred_element_type=F32)
        w = weights(kappa, gram, rowv[0, rsl, :], rowv[1, rsl, :],
                    src_info[start:start + 1, :], src_info[block_chunks + start:block_chunks + start + 1, :])
        sums = sv[rsl, :] + w
        wv[rsl, half * CHUNK:(half + 1) * CHUNK] = w.astype(jnp.bfloat16)
        sv[rsl, :] = sums
        if half:
            for g in range(SUB_ROWS // 8):
                acc = acc + sums[g * 8:(g + 1) * 8]
        return acc

    part = lax.fori_loop(0, xv.shape[0] // SUB_ROWS, row_tile, jnp.zeros((8, 128), F32))
    if half:
        refs[8][...] = part


def last_step(x, rowf, src_info, cols, start, carry, half):
    rows, width = x.shape
    ins = [x, rowf, src_info, cols, *carry]
    part_shape = [jax.ShapeDtypeStruct((8, 128), F32)] if half else []
    return pl.pallas_call(
        functools.partial(last_kernel, (start, half, LOG2E * 0.5 / width)),
        out_shape=[pltpu.VMEM((rows, 128), F32), pltpu.VMEM((rows, 2 * CHUNK), jnp.bfloat16)] + part_shape,
        in_specs=[VMEM_SPEC] * len(ins), out_specs=[VMEM_SPEC] * (2 + len(part_shape)),
        input_output_aliases={4 + k: k for k in range(len(carry))},
        compiler_params=pltpu.CompilerParams(vmem_limit_bytes=VMEM_LIMIT),
        cost_estimate=pl.CostEstimate(flops=2 * rows * CHUNK * width, bytes_accessed=rows * width, transcendentals=0))(*ins)


def finish_kernel(inv_len2, xv, tv, sv, wv, cols_a, cols_b, my_info, blank, forces, xc, buf, out_sems):
    del blank
    xc[:CHUNK, :] = cols_a[...]
    xc[CHUNK:, :] = cols_b[...]
    num = live_tiles(my_info)

    def out(i):
        return pltpu.make_async_copy(
            buf.at[lax.rem(i, 4)], forces.at[pl.ds(pl.multiple_of(i * FINISH_TILE, FINISH_TILE), FINISH_TILE)], out_sems.at[lax.rem(i, 4)])

    def one(i, _):
        @pl.when(i >= 4)
        def _():
            out(i - 4).wait()

        sl = pl.ds(pl.multiple_of(i * FINISH_TILE, FINISH_TILE), FINISH_TILE)
        total = jnp.sum(sv[sl, :], axis=1, keepdims=True)
        pulled = tv[sl, :] + jnp.dot(wv[sl, :], xc[...], preferred_element_type=F32)
        buf[lax.rem(i, 4)] = (total * xv[sl, :].astype(F32) - pulled) * inv_len2
        out(i).start()
        return 0

    lax.fori_loop(0, num, one, 0)

    def drain(i, _):
        out(i).wait()
        return 0

    lax.fori_loop(jnp.maximum(num - 4, 0), num, drain, 0)


def finish(*ins):
    x = ins[0]
    rows, width = x.shape
    return pl.pallas_call(
        functools.partial(finish_kernel, 1.0 / width),
        out_shape=jax.ShapeDtypeStruct((rows, width), F32),
        in_specs=[VMEM_SPEC] * (len(ins) - 1) + [HBM_SPEC], out_specs=HBM_SPEC,
        scratch_shapes=[pltpu.VMEM((2 * CHUNK, width), x.dtype), pltpu.VMEM((4, FINISH_TILE, width), F32),
                        pltpu.SemaphoreType.DMA((4,))],
        input_output_aliases={len(ins) - 1: 0},
        compiler_params=pltpu.CompilerParams(vmem_limit_bytes=VMEM_LIMIT),
        cost_estimate=pl.CostEstimate(flops=rows * width * 1000, bytes_accessed=rows * width * 4, transcendentals=0),
        name='finish')(*ins)


VMEM_LIMIT = 24 * 1024 * 1024


def step(x, rowf, my_info, src_info, cols, start, num, tile_chunks, carry):
    rows, width = x.shape
    first, diag = carry is None, cols is None
    cfg = (start, num, tile_chunks, first, diag, LOG2E * 0.5 / width)
    ins = [x, rowf, my_info] + ([] if diag else [src_info, cols]) + ([] if first else list(carry))
    in_specs = [VMEM_SPEC] * len(ins)
    flops = int(4 * rows * num * CHUNK * width * 0.6)
    common = dict(
        in_specs=in_specs,
        compiler_params=pltpu.CompilerParams(vmem_limit_bytes=VMEM_LIMIT),
        cost_estimate=pl.CostEstimate(flops=flops, bytes_accessed=rows * width, transcendentals=0),
        name='step_%d_%d' % (start, num))
    kernel = functools.partial(step_kernel, cfg)
    return pl.pallas_call(
        kernel,
        out_shape=[pltpu.VMEM((rows, width), F32), pltpu.VMEM((rows, 128), F32)],
        out_specs=[VMEM_SPEC] * 2,
        input_output_aliases={} if first else {len(ins) - 2: 0, len(ins) - 1: 1}, **common)(*ins)


PIECES = (512, 512, 512, 256, 128, 128)


def solution(mesh):
    num_blocks = mesh.shape['row']
    cross_perm = [(src, src ^ 2) for src in range(num_blocks)]
    pair_perm = [(src, src ^ 1) for src in range(num_blocks)]
    diag_perm = [(src, src ^ 3) for src in range(num_blocks)]

    def per_device(positions, charges, counts):
        rows, _ = positions.shape
        chunks = rows // CHUNK
        raw = pltpu.with_memory_space_constraint(positions, pltpu.VMEM)
        head = jnp.where(jnp.arange(PIECES[0])[:, None] < counts[0], positions[:PIECES[0]], 0)
        arrived = [lax.ppermute(head, 'row', cross_perm)]
        x, rowf, info, blank = prep(raw, charges, counts)
        info_cross = lax.ppermute(info, 'row', cross_perm)
        info_pair = lax.ppermute(info, 'row', pair_perm)
        off = PIECES[0]
        for size in PIECES[1:]:
            arrived.append(lax.ppermute(x[off:off + size], 'row', cross_perm))
            off += size
        partner = lax.ppermute(x, 'row', pair_perm)
        carry = step(x, rowf, info, None, None, 0, chunks, 4, None)
        partner, *carry = lax.optimization_barrier((partner, *carry))
        carry = step(x, rowf, info, info_pair, partner, 0, chunks, 4, carry)
        info_cross, *carry = lax.optimization_barrier((info_cross, *carry))
        info_diag = lax.ppermute(info_cross, 'row', pair_perm)
        off = 0
        for k, piece in enumerate(arrived):
            num = PIECES[k] // CHUNK
            piece, *carry = lax.optimization_barrier((piece, *carry))
            relay = lax.ppermute(piece, 'row', pair_perm)
            if num > 1:
                carry = step(x, rowf, info, info_cross, piece, off, num, min(4, num), carry)
                carry = step(x, rowf, info, info_diag, relay, off, num, min(4, num), carry)
            elif k < len(PIECES) - 1:
                carry = pair_step(x, rowf, (info_cross, info_diag), (piece, relay), off, carry)
            else:
                t_sum, s_sum = carry
                carry = last_step(x, rowf, info_cross, piece, off, (s_sum,), 0)
                s_sum, w_last, part = last_step(x, rowf, info_diag, relay, off, carry, 1)
            off += num
        total = part
        for perm in (cross_perm, pair_perm, diag_perm):
            total = total + lax.ppermute(part, 'row', perm)
        forces = finish(x, t_sum, s_sum, w_last, piece, relay, info, blank)
        return forces, (0.5 * jnp.sum(total)).reshape(1)

    row_spec = P(('sys', 'row'), None)
    vec_spec = P(('sys', 'row'))
    return jax.shard_map(per_device, mesh=mesh, in_specs=(row_spec, vec_spec, vec_spec), out_specs=(row_spec, P('sys')), check_vma=False)
```

```python
import functools

import jax
import jax.numpy as jnp
from jax import lax
from jax.experimental import pallas as pl
from jax.experimental.pallas import tpu as pltpu
from jax.sharding import PartitionSpec as P


CHUNK = 128
SUB_ROWS = 512
LOG2E = 1.4426950408889634
F32 = jnp.float32
VMEM_SPEC = pl.BlockSpec(memory_space=pltpu.VMEM)
HBM_SPEC = pl.BlockSpec(memory_space=pl.ANY)
FINISH_TILE = 256


def count_of(info_ref):
    return jnp.max(info_ref[info_ref.shape[0] - 8:, :]).astype(jnp.int32)


def live_tiles(info_ref):
    return (count_of(info_ref) + FINISH_TILE - 1) // FINISH_TILE


def prep_kernel(kappa, raw_hbm, q_hbm, count_ref, xv, rowv, info, forces, zeros, q_ref, sem, in_sems):
    rows = raw_hbm.shape[0]
    chunks = rows // CHUNK
    eye = lax.broadcasted_iota(jnp.int32, (CHUNK, CHUNK), 0) == lax.broadcasted_iota(jnp.int32, (CHUNK, CHUNK), 1)
    lane = lax.broadcasted_iota(jnp.int32, (1, CHUNK), 1)
    count = count_ref[0]
    group = rows // 4
    charge_copy = pltpu.make_async_copy(q_hbm, q_ref, in_sems.at[4])
    charge_copy.start()

    def fetch(g):
        return pltpu.make_async_copy(raw_hbm.at[pl.ds(g * group, group)], xv.at[pl.ds(g * group, group)], in_sems.at[g])

    for g in range(4):
        fetch(g).start()
    tiles = rows // FINISH_TILE
    live = (count + FINISH_TILE - 1) // FINISH_TILE
    zeros[...] = jnp.zeros_like(zeros)

    def blank(i):
        return pltpu.make_async_copy(zeros, forces.at[pl.ds(pl.multiple_of(i * FINISH_TILE, FINISH_TILE), FINISH_TILE)], sem)

    def start(i, _):
        blank(i).start()
        return 0

    lax.fori_loop(live, tiles, start, 0)
    info[2 * chunks:, :] = jnp.full((8, CHUNK), count, jnp.int32).astype(F32)

    def one(c, _):
        sl = pl.ds(pl.multiple_of(c * CHUNK, CHUNK), CHUNK)
        row_ids = lax.broadcasted_iota(jnp.int32, (CHUNK, 1), 0) + c * CHUNK
        block = jnp.where(row_ids < count, xv[sl, :].astype(F32), 0.0)
        xv[sl, :] = block.astype(xv.dtype)
        col_s = -kappa * jnp.sum(block * block, axis=1, keepdims=True)
        rowv[0, sl, :] = jnp.broadcast_to(col_s, (CHUNK, CHUNK))
        info[pl.ds(c, 1), :] = jnp.sum(jnp.where(eye, col_s, 0.0), axis=0, keepdims=True)
        live = jnp.where(lane + c * CHUNK < count, q_ref[pl.ds(c, 1), :], 0.0)
        info[pl.ds(chunks + c, 1), :] = live
        rowv[1, sl, :] = jnp.broadcast_to(jnp.sum(jnp.where(eye, live, 0.0), axis=1, keepdims=True), (CHUNK, CHUNK))
        return 0

    charge_copy.wait()
    for g in range(4):
        fetch(g).wait()
        lax.fori_loop(g * chunks // 4, (g + 1) * chunks // 4, one, 0)

    def wait(i, _):
        blank(i).wait()
        return 0

    lax.fori_loop(live, tiles, wait, 0)


def prep(x, charges, counts):
    rows, width = x.shape
    chunks = rows // CHUNK
    return pl.pallas_call(
        functools.partial(prep_kernel, LOG2E * 0.5 / width),
        out_shape=[jax.ShapeDtypeStruct(x.shape, x.dtype), pltpu.VMEM((2, rows, CHUNK), F32),
                   jax.ShapeDtypeStruct((2 * chunks + 8, CHUNK), F32), jax.ShapeDtypeStruct((rows, width), F32)],
        in_specs=[pl.BlockSpec(memory_space=pltpu.HBM)] * 2 + [pl.BlockSpec(memory_space=pltpu.SMEM)], out_specs=[VMEM_SPEC] * 3 + [HBM_SPEC],
        scratch_shapes=[pltpu.VMEM((FINISH_TILE, width), F32), pltpu.VMEM((chunks, CHUNK), F32), pltpu.SemaphoreType.DMA,
                        pltpu.SemaphoreType.DMA((5,))],
        compiler_params=pltpu.CompilerParams(vmem_limit_bytes=VMEM_LIMIT),
        name='prep')(x, charges.reshape(chunks, CHUNK), counts)


def weights(kappa, gram, row_a, row_c, col_a, col_c):
    expo = jnp.minimum(gram * (2.0 * kappa) + row_a + col_a, 0.0)
    return jnp.exp2(expo) * (row_c * col_c)


def step_kernel(cfg, *refs):
    start, num, tile_chunks, first, diag, kappa = cfg
    refs = list(refs)
    xv, rowv, my_info = refs[:3]
    refs = refs[3:]
    cols, src_info = xv, my_info
    if not diag:
        src_info, cols = refs[:2]
        refs = refs[2:]
    if not first:
        refs = refs[2:]
    tv, sv = refs[:2]
    rows, _ = xv.shape
    block_chunks = rows // CHUNK
    col_tile = tile_chunks * CHUNK
    live = jnp.clip((count_of(src_info) + CHUNK - 1) // CHUNK - start, 0, num)
    tiles = (live + tile_chunks - 1) // tile_chunks

    def old(ref, ct, rsl):
        return jnp.where(ct == 0, 0.0, ref[rsl, :]) if first else ref[rsl, :]

    def weigh(ct, c0, r0):
        rsl = pl.ds(r0, SUB_ROWS)
        s_sum = old(sv, ct, rsl)
        row_a = rowv[0, rsl, :]
        row_c = rowv[1, rsl, :]
        parts = []
        for q in range(tile_chunks // 2):
            gram = lax.dot_general(xv[rsl, :], cols[pl.ds(c0 + q * 256, 256), :], (((1,), (1,)), ((), ())),
                                   preferred_element_type=F32)
            for h in range(2):
                k = 2 * q + h
                cid = start + ct * tile_chunks + k
                col_a = src_info[pl.ds(cid, 1), :]
                col_c = src_info[pl.ds(block_chunks + cid, 1), :]
                w = weights(kappa, gram[:, h * 128:(h + 1) * 128], row_a, row_c, col_a, col_c)
                if diag:
                    delta = lax.broadcasted_iota(jnp.int32, w.shape, 0) - lax.broadcasted_iota(jnp.int32, w.shape, 1)
                    w = jnp.where(delta == c0 + k * CHUNK - r0, 0.0, w)
                s_sum = s_sum + w
                parts.append(w.astype(jnp.bfloat16))
        sv[rsl, :] = s_sum
        return jnp.concatenate(parts, axis=1)

    def pull(w, ct, c0, r0):
        rsl = pl.ds(r0, SUB_ROWS)
        tv[rsl, :] = old(tv, ct, rsl) + jnp.dot(w, cols[pl.ds(c0, col_tile), :], preferred_element_type=F32)

    def tile(ct, _):
        c0 = pl.multiple_of(ct * col_tile, col_tile)
        w = None
        for r0 in range(0, rows, SUB_ROWS):
            w_next = weigh(ct, c0, r0)
            if w is not None:
                pull(w, ct, c0, r0 - SUB_ROWS)
            w = w_next
        pull(w, ct, c0, rows - SUB_ROWS)
        return 0

    lax.fori_loop(0, tiles, tile, 0)


def last_kernel(cfg, xv, rowv, src_info, cols, s_in, sv, wv, part):
    start, num, kappa = cfg
    block_chunks = xv.shape[0] // CHUNK

    def row_tile(rt, acc):
        rsl = pl.ds(pl.multiple_of(rt * SUB_ROWS, SUB_ROWS), SUB_ROWS)
        gram = lax.dot_general(xv[rsl, :], cols[...], (((1,), (1,)), ((), ())), preferred_element_type=F32)
        sums = sv[rsl, :]
        for k in range(num):
            w = weights(kappa, gram[:, k * CHUNK:(k + 1) * CHUNK], rowv[0, rsl, :], rowv[1, rsl, :],
                        src_info[start + k:start + k + 1, :], src_info[block_chunks + start + k:block_chunks + start + k + 1, :])
            sums = sums + w
            wv[rsl, k * CHUNK:(k + 1) * CHUNK] = w.astype(jnp.bfloat16)
        sv[rsl, :] = sums
        for g in range(SUB_ROWS // 8):
            acc = acc + sums[g * 8:(g + 1) * 8]
        return acc

    part[...] = lax.fori_loop(0, xv.shape[0] // SUB_ROWS, row_tile, jnp.zeros((8, 128), F32))


def last_step(x, rowf, src_info, cols, start, s_sum):
    rows, width = x.shape
    num = cols.shape[0] // CHUNK
    ins = [x, rowf, src_info, cols, s_sum]
    return pl.pallas_call(
        functools.partial(last_kernel, (start, num, LOG2E * 0.5 / width)),
        out_shape=[pltpu.VMEM((rows, 128), F32), pltpu.VMEM((rows, num * CHUNK), jnp.bfloat16), jax.ShapeDtypeStruct((8, 128), F32)],
        in_specs=[VMEM_SPEC] * len(ins), out_specs=[VMEM_SPEC] * 3,
        input_output_aliases={4: 0},
        compiler_params=pltpu.CompilerParams(vmem_limit_bytes=VMEM_LIMIT),
        cost_estimate=pl.CostEstimate(flops=2 * rows * num * CHUNK * width, bytes_accessed=rows * width, transcendentals=0),
        name='last')(*ins)


def finish_kernel(inv_len2, xv, tv, sv, wv, cols, my_info, blank, forces, buf, out_sems):
    del blank
    num = live_tiles(my_info)

    def out(i):
        return pltpu.make_async_copy(
            buf.at[lax.rem(i, 4)], forces.at[pl.ds(pl.multiple_of(i * FINISH_TILE, FINISH_TILE), FINISH_TILE)], out_sems.at[lax.rem(i, 4)])

    def one(i, _):
        @pl.when(i >= 4)
        def _():
            out(i - 4).wait()

        sl = pl.ds(pl.multiple_of(i * FINISH_TILE, FINISH_TILE), FINISH_TILE)
        total = jnp.sum(sv[sl, :], axis=1, keepdims=True)
        pulled = tv[sl, :] + jnp.dot(wv[sl, :], cols[...], preferred_element_type=F32)
        buf[lax.rem(i, 4)] = (total * xv[sl, :].astype(F32) - pulled) * inv_len2
        out(i).start()
        return 0

    lax.fori_loop(0, num, one, 0)

    def drain(i, _):
        out(i).wait()
        return 0

    lax.fori_loop(jnp.maximum(num - 4, 0), num, drain, 0)


def finish(*ins):
    x = ins[0]
    rows, width = x.shape
    return pl.pallas_call(
        functools.partial(finish_kernel, 1.0 / width),
        out_shape=jax.ShapeDtypeStruct((rows, width), F32),
        in_specs=[VMEM_SPEC] * (len(ins) - 1) + [HBM_SPEC], out_specs=HBM_SPEC,
        scratch_shapes=[pltpu.VMEM((4, FINISH_TILE, width), F32), pltpu.SemaphoreType.DMA((4,))],
        input_output_aliases={len(ins) - 1: 0},
        compiler_params=pltpu.CompilerParams(vmem_limit_bytes=VMEM_LIMIT),
        cost_estimate=pl.CostEstimate(flops=rows * width * 1000, bytes_accessed=rows * width * 4, transcendentals=0),
        name='finish')(*ins)


VMEM_LIMIT = 24 * 1024 * 1024


def step(x, rowf, my_info, src_info, cols, start, num, tile_chunks, carry):
    rows, width = x.shape
    first, diag = carry is None, cols is None
    cfg = (start, num, tile_chunks, first, diag, LOG2E * 0.5 / width)
    ins = [x, rowf, my_info] + ([] if diag else [src_info, cols]) + ([] if first else list(carry))
    in_specs = [VMEM_SPEC] * len(ins)
    flops = int(4 * rows * num * CHUNK * width * 0.6)
    common = dict(
        in_specs=in_specs,
        compiler_params=pltpu.CompilerParams(vmem_limit_bytes=VMEM_LIMIT),
        cost_estimate=pl.CostEstimate(flops=flops, bytes_accessed=rows * width, transcendentals=0),
        name='step_%d_%d' % (start, num))
    kernel = functools.partial(step_kernel, cfg)
    return pl.pallas_call(
        kernel,
        out_shape=[pltpu.VMEM((rows, width), F32), pltpu.VMEM((rows, 128), F32)],
        out_specs=[VMEM_SPEC] * 2,
        input_output_aliases={} if first else {len(ins) - 2: 0, len(ins) - 1: 1}, **common)(*ins)


PIECES = (512, 512, 512, 256, 256)


def solution(mesh):
    num_blocks = mesh.shape['row']
    cross_perm = [(src, src ^ 2) for src in range(num_blocks)]
    pair_perm = [(src, src ^ 1) for src in range(num_blocks)]
    diag_perm = [(src, src ^ 3) for src in range(num_blocks)]

    def per_device(positions, charges, counts):
        rows, _ = positions.shape
        chunks = rows // CHUNK
        head = jnp.where(jnp.arange(PIECES[0])[:, None] < counts[0], positions[:PIECES[0]], 0)
        arrived = [lax.ppermute(head, 'row', cross_perm)]
        x, rowf, info, blank = prep(positions, charges, counts)
        info_cross = lax.ppermute(info, 'row', cross_perm)
        info_pair = lax.ppermute(info, 'row', pair_perm)
        off = PIECES[0]
        for size in PIECES[1:]:
            arrived.append(lax.ppermute(x[off:off + size], 'row', cross_perm))
            off += size
        partner = lax.ppermute(x, 'row', pair_perm)
        carry = step(x, rowf, info, None, None, 0, chunks, 4, None)
        partner, *carry = lax.optimization_barrier((partner, *carry))
        carry = step(x, rowf, info, info_pair, partner, 0, chunks, 4, carry)
        info_cross, *carry = lax.optimization_barrier((info_cross, *carry))
        info_diag = lax.ppermute(info_cross, 'row', pair_perm)
        off = 0
        for k, piece in enumerate(arrived):
            num = PIECES[k] // CHUNK
            piece, *carry = lax.optimization_barrier((piece, *carry))
            relay = lax.ppermute(piece, 'row', pair_perm)
            carry = step(x, rowf, info, info_cross, piece, off, num, min(4, num), carry)
            if k < len(PIECES) - 1:
                carry = step(x, rowf, info, info_diag, relay, off, num, min(4, num), carry)
            else:
                t_sum, s_sum = carry
                s_sum, w_last, part = last_step(x, rowf, info_diag, relay, off, s_sum)
            off += num
        total = part
        for perm in (cross_perm, pair_perm, diag_perm):
            total = total + lax.ppermute(part, 'row', perm)
        forces = finish(x, t_sum, s_sum, w_last, relay, info, blank)
        return forces, (0.5 * jnp.sum(total)).reshape(1)

    row_spec = P(('sys', 'row'), None)
    vec_spec = P(('sys', 'row'))
    return jax.shard_map(per_device, mesh=mesh, in_specs=(row_spec, vec_spec, vec_spec), out_specs=(row_spec, P('sys')), check_vma=False)
```

```python
import functools

import jax
import jax.numpy as jnp
from jax import lax
from jax.experimental import pallas as pl
from jax.experimental.pallas import tpu as pltpu
from jax.sharding import PartitionSpec as P


CHUNK = 128
SUB_ROWS = 512
LOG2E = 1.4426950408889634
F32 = jnp.float32
VMEM_SPEC = pl.BlockSpec(memory_space=pltpu.VMEM)
HBM_SPEC = pl.BlockSpec(memory_space=pl.ANY)
FINISH_TILE = 256


def count_of(info_ref):
    return jnp.max(info_ref[info_ref.shape[0] - 8:, :]).astype(jnp.int32)


def live_tiles(info_ref):
    return (count_of(info_ref) + FINISH_TILE - 1) // FINISH_TILE


def prep_kernel(kappa, raw_hbm, q_hbm, count_ref, xv, rowv, info, forces, zeros, q_ref, sem, in_sems):
    rows = raw_hbm.shape[0]
    chunks = rows // CHUNK
    eye = lax.broadcasted_iota(jnp.int32, (CHUNK, CHUNK), 0) == lax.broadcasted_iota(jnp.int32, (CHUNK, CHUNK), 1)
    lane = lax.broadcasted_iota(jnp.int32, (1, CHUNK), 1)
    count = count_ref[0]
    group = rows // 4
    charge_copy = pltpu.make_async_copy(q_hbm, q_ref, in_sems.at[4])
    charge_copy.start()

    def fetch(g):
        return pltpu.make_async_copy(raw_hbm.at[pl.ds(g * group, group)], xv.at[pl.ds(g * group, group)], in_sems.at[g])

    for g in range(4):
        fetch(g).start()
    tiles = rows // FINISH_TILE
    live = (count + FINISH_TILE - 1) // FINISH_TILE
    zeros[...] = jnp.zeros_like(zeros)

    def blank(i):
        return pltpu.make_async_copy(zeros, forces.at[pl.ds(pl.multiple_of(i * FINISH_TILE, FINISH_TILE), FINISH_TILE)], sem)

    def start(i, _):
        blank(i).start()
        return 0

    lax.fori_loop(live, tiles, start, 0)
    info[2 * chunks:, :] = jnp.full((8, CHUNK), count, jnp.int32).astype(F32)

    def one(c, _):
        sl = pl.ds(pl.multiple_of(c * CHUNK, CHUNK), CHUNK)
        row_ids = lax.broadcasted_iota(jnp.int32, (CHUNK, 1), 0) + c * CHUNK
        block = jnp.where(row_ids < count, xv[sl, :].astype(F32), 0.0)
        xv[sl, :] = block.astype(xv.dtype)
        col_s = -kappa * jnp.sum(block * block, axis=1, keepdims=True)
        rowv[0, sl, :] = jnp.broadcast_to(col_s, (CHUNK, CHUNK))
        info[pl.ds(c, 1), :] = jnp.sum(jnp.where(eye, col_s, 0.0), axis=0, keepdims=True)
        live = jnp.where(lane + c * CHUNK < count, q_ref[pl.ds(c, 1), :], 0.0)
        info[pl.ds(chunks + c, 1), :] = live
        rowv[1, sl, :] = jnp.broadcast_to(jnp.sum(jnp.where(eye, live, 0.0), axis=1, keepdims=True), (CHUNK, CHUNK))
        return 0

    charge_copy.wait()
    for g in range(4):
        fetch(g).wait()
        lax.fori_loop(g * chunks // 4, (g + 1) * chunks // 4, one, 0)

    def wait(i, _):
        blank(i).wait()
        return 0

    lax.fori_loop(live, tiles, wait, 0)


def prep(x, charges, counts):
    rows, width = x.shape
    chunks = rows // CHUNK
    return pl.pallas_call(
        functools.partial(prep_kernel, LOG2E * 0.5 / width),
        out_shape=[jax.ShapeDtypeStruct(x.shape, x.dtype), pltpu.VMEM((2, rows, CHUNK), F32),
                   jax.ShapeDtypeStruct((2 * chunks + 8, CHUNK), F32), jax.ShapeDtypeStruct((rows, width), F32)],
        in_specs=[pl.BlockSpec(memory_space=pltpu.HBM)] * 2 + [pl.BlockSpec(memory_space=pltpu.SMEM)], out_specs=[VMEM_SPEC] * 3 + [HBM_SPEC],
        scratch_shapes=[pltpu.VMEM((FINISH_TILE, width), F32), pltpu.VMEM((chunks, CHUNK), F32), pltpu.SemaphoreType.DMA,
                        pltpu.SemaphoreType.DMA((5,))],
        compiler_params=pltpu.CompilerParams(vmem_limit_bytes=VMEM_LIMIT),
        name='prep')(x, charges.reshape(chunks, CHUNK), counts)


def weights(kappa, gram, row_a, row_c, col_a, col_c):
    expo = jnp.minimum(gram * (2.0 * kappa) + row_a + col_a, 0.0)
    return jnp.exp2(expo) * (row_c * col_c)


def step_kernel(cfg, *refs):
    start, num, tile_chunks, first, diag, kappa = cfg
    refs = list(refs)
    xv, rowv, my_info = refs[:3]
    refs = refs[3:]
    cols, src_info = xv, my_info
    if not diag:
        src_info, cols = refs[:2]
        refs = refs[2:]
    if not first:
        refs = refs[2:]
    tv, sv = refs[:2]
    rows, _ = xv.shape
    block_chunks = rows // CHUNK
    col_tile = tile_chunks * CHUNK
    live = jnp.clip((count_of(src_info) + CHUNK - 1) // CHUNK - start, 0, num)
    tiles = (live + tile_chunks - 1) // tile_chunks

    def old(ref, ct, rsl):
        return jnp.where(ct == 0, 0.0, ref[rsl, :]) if first else ref[rsl, :]

    def weigh(ct, c0, r0):
        rsl = pl.ds(r0, SUB_ROWS)
        s_sum = old(sv, ct, rsl)
        row_a = rowv[0, rsl, :]
        row_c = rowv[1, rsl, :]
        parts = []
        for q in range(tile_chunks // 2):
            gram = lax.dot_general(xv[rsl, :], cols[pl.ds(c0 + q * 256, 256), :], (((1,), (1,)), ((), ())),
                                   preferred_element_type=F32)
            for h in range(2):
                k = 2 * q + h
                cid = start + ct * tile_chunks + k
                col_a = src_info[pl.ds(cid, 1), :]
                col_c = src_info[pl.ds(block_chunks + cid, 1), :]
                w = weights(kappa, gram[:, h * 128:(h + 1) * 128], row_a, row_c, col_a, col_c)
                if diag:
                    delta = lax.broadcasted_iota(jnp.int32, w.shape, 0) - lax.broadcasted_iota(jnp.int32, w.shape, 1)
                    w = jnp.where(delta == c0 + k * CHUNK - r0, 0.0, w)
                s_sum = s_sum + w
                parts.append(w.astype(jnp.bfloat16))
        sv[rsl, :] = s_sum
        return jnp.concatenate(parts, axis=1)

    def pull(w, ct, c0, r0):
        rsl = pl.ds(r0, SUB_ROWS)
        tv[rsl, :] = old(tv, ct, rsl) + jnp.dot(w, cols[pl.ds(c0, col_tile), :], preferred_element_type=F32)

    def tile(ct, _):
        c0 = pl.multiple_of(ct * col_tile, col_tile)
        w = None
        for r0 in range(0, rows, SUB_ROWS):
            w_next = weigh(ct, c0, r0)
            if w is not None:
                pull(w, ct, c0, r0 - SUB_ROWS)
            w = w_next
        pull(w, ct, c0, rows - SUB_ROWS)
        return 0

    lax.fori_loop(0, tiles, tile, 0)


def last_kernel(cfg, *refs):
    start, num, half, kappa = cfg
    xv, rowv, src_info, cols = refs[:4]
    sv, wv = refs[6:8] if half else refs[5:7]
    block_chunks = xv.shape[0] // CHUNK
    acc = jnp.zeros((8, 128), F32)
    for r0 in range(0, xv.shape[0], SUB_ROWS):
        rsl = pl.ds(r0, SUB_ROWS)
        gram = lax.dot_general(xv[rsl, :], cols[...], (((1,), (1,)), ((), ())), preferred_element_type=F32)
        sums = sv[rsl, :]
        for k in range(num):
            w = weights(kappa, gram[:, k * CHUNK:(k + 1) * CHUNK], rowv[0, rsl, :], rowv[1, rsl, :],
                        src_info[start + k:start + k + 1, :], src_info[block_chunks + start + k:block_chunks + start + k + 1, :])
            sums = sums + w
            wv[rsl, (half * num + k) * CHUNK:(half * num + k + 1) * CHUNK] = w.astype(jnp.bfloat16)
        sv[rsl, :] = sums
        if half:
            for g in range(SUB_ROWS // 8):
                acc = acc + sums[g * 8:(g + 1) * 8]
    if half:
        refs[8][...] = acc


def last_step(x, rowf, src_info, cols, start, carry, half):
    rows, width = x.shape
    num = cols.shape[0] // CHUNK
    ins = [x, rowf, src_info, cols, *carry]
    part_shape = [jax.ShapeDtypeStruct((8, 128), F32)] if half else []
    return pl.pallas_call(
        functools.partial(last_kernel, (start, num, half, LOG2E * 0.5 / width)),
        out_shape=[pltpu.VMEM((rows, 128), F32), pltpu.VMEM((rows, 2 * num * CHUNK), jnp.bfloat16)] + part_shape,
        in_specs=[VMEM_SPEC] * len(ins), out_specs=[VMEM_SPEC] * (2 + len(part_shape)),
        input_output_aliases={4 + k: k for k in range(len(carry))},
        compiler_params=pltpu.CompilerParams(vmem_limit_bytes=VMEM_LIMIT),
        cost_estimate=pl.CostEstimate(flops=2 * rows * num * CHUNK * width, bytes_accessed=rows * width, transcendentals=0))(*ins)


def finish_kernel(inv_len2, xv, tv, sv, wv, cols_a, cols_b, my_info, blank, forces, cols, buf, out_sems):
    del blank
    num = live_tiles(my_info)
    half = cols_a.shape[0]
    cols[:half, :] = cols_a[...]
    cols[half:, :] = cols_b[...]

    def out(i):
        return pltpu.make_async_copy(
            buf.at[lax.rem(i, 4)], forces.at[pl.ds(pl.multiple_of(i * FINISH_TILE, FINISH_TILE), FINISH_TILE)], out_sems.at[lax.rem(i, 4)])

    def one(i, _):
        @pl.when(i >= 4)
        def _():
            out(i - 4).wait()

        sl = pl.ds(pl.multiple_of(i * FINISH_TILE, FINISH_TILE), FINISH_TILE)
        total = jnp.sum(sv[sl, :], axis=1, keepdims=True)
        pulled = tv[sl, :] + jnp.dot(wv[sl, :], cols[...], preferred_element_type=F32)
        buf[lax.rem(i, 4)] = (total * xv[sl, :].astype(F32) - pulled) * inv_len2
        out(i).start()
        return 0

    lax.fori_loop(0, num, one, 0)

    def drain(i, _):
        out(i).wait()
        return 0

    lax.fori_loop(jnp.maximum(num - 4, 0), num, drain, 0)


def finish(*ins):
    x = ins[0]
    rows, width = x.shape
    return pl.pallas_call(
        functools.partial(finish_kernel, 1.0 / width),
        out_shape=jax.ShapeDtypeStruct((rows, width), F32),
        in_specs=[VMEM_SPEC] * (len(ins) - 1) + [HBM_SPEC], out_specs=HBM_SPEC,
        scratch_shapes=[pltpu.VMEM((2 * ins[4].shape[0], width), x.dtype), pltpu.VMEM((4, FINISH_TILE, width), F32), pltpu.SemaphoreType.DMA((4,))],
        input_output_aliases={len(ins) - 1: 0},
        compiler_params=pltpu.CompilerParams(vmem_limit_bytes=VMEM_LIMIT),
        cost_estimate=pl.CostEstimate(flops=rows * width * 1000, bytes_accessed=rows * width * 4, transcendentals=0),
        name='finish')(*ins)


VMEM_LIMIT = 24 * 1024 * 1024


def step(x, rowf, my_info, src_info, cols, start, num, tile_chunks, carry):
    rows, width = x.shape
    first, diag = carry is None, cols is None
    cfg = (start, num, tile_chunks, first, diag, LOG2E * 0.5 / width)
    ins = [x, rowf, my_info] + ([] if diag else [src_info, cols]) + ([] if first else list(carry))
    in_specs = [VMEM_SPEC] * len(ins)
    flops = int(4 * rows * num * CHUNK * width * 0.6)
    common = dict(
        in_specs=in_specs,
        compiler_params=pltpu.CompilerParams(vmem_limit_bytes=VMEM_LIMIT),
        cost_estimate=pl.CostEstimate(flops=flops, bytes_accessed=rows * width, transcendentals=0),
        name='step_%d_%d' % (start, num))
    kernel = functools.partial(step_kernel, cfg)
    return pl.pallas_call(
        kernel,
        out_shape=[pltpu.VMEM((rows, width), F32), pltpu.VMEM((rows, 128), F32)],
        out_specs=[VMEM_SPEC] * 2,
        input_output_aliases={} if first else {len(ins) - 2: 0, len(ins) - 1: 1}, **common)(*ins)


PIECES = (256, 512, 512, 512, 256)


def solution(mesh):
    num_blocks = mesh.shape['row']
    cross_perm = [(src, src ^ 2) for src in range(num_blocks)]
    pair_perm = [(src, src ^ 1) for src in range(num_blocks)]
    diag_perm = [(src, src ^ 3) for src in range(num_blocks)]

    def per_device(positions, charges, counts):
        rows, _ = positions.shape
        chunks = rows // CHUNK
        head = jnp.where(jnp.arange(PIECES[0])[:, None] < counts[0], positions[:PIECES[0]], 0)
        arrived = [lax.ppermute(head, 'row', cross_perm)]
        x, rowf, info, blank = prep(positions, charges, counts)
        info_cross = lax.ppermute(info, 'row', cross_perm)
        info_pair = lax.ppermute(info, 'row', pair_perm)
        off = PIECES[0]
        for size in PIECES[1:]:
            arrived.append(lax.ppermute(x[off:off + size], 'row', cross_perm))
            off += size
        partner = lax.ppermute(x, 'row', pair_perm)
        carry = step(x, rowf, info, None, None, 0, chunks, 4, None)
        partner, *carry = lax.optimization_barrier((partner, *carry))
        carry = step(x, rowf, info, info_pair, partner, 0, chunks, 4, carry)
        info_cross, *carry = lax.optimization_barrier((info_cross, *carry))
        info_diag = lax.ppermute(info_cross, 'row', pair_perm)
        off = 0
        for k, piece in enumerate(arrived):
            num = PIECES[k] // CHUNK
            piece, *carry = lax.optimization_barrier((piece, *carry))
            relay = lax.ppermute(piece, 'row', pair_perm)
            if k < len(PIECES) - 1:
                carry = step(x, rowf, info, info_cross, piece, off, num, min(4, num), carry)
                carry = step(x, rowf, info, info_diag, relay, off, num, min(4, num), carry)
            else:
                t_sum, s_sum = carry
                carry = last_step(x, rowf, info_cross, piece, off, (s_sum,), 0)
                s_sum, w_last, part = last_step(x, rowf, info_diag, relay, off, carry, 1)
            off += num
        total = part
        for perm in (cross_perm, pair_perm, diag_perm):
            total = total + lax.ppermute(part, 'row', perm)
        forces = finish(x, t_sum, s_sum, w_last, piece, relay, info, blank)
        return forces, (0.5 * jnp.sum(total)).reshape(1)

    row_spec = P(('sys', 'row'), None)
    vec_spec = P(('sys', 'row'))
    return jax.shard_map(per_device, mesh=mesh, in_specs=(row_spec, vec_spec, vec_spec), out_specs=(row_spec, P('sys')), check_vma=False)
```

```python
import functools

import jax
import jax.numpy as jnp
from jax import lax
from jax.experimental import pallas as pl
from jax.experimental.pallas import tpu as pltpu
from jax.sharding import PartitionSpec as P


CHUNK = 128
SUB_ROWS = 512
LOG2E = 1.4426950408889634
F32 = jnp.float32
VMEM_SPEC = pl.BlockSpec(memory_space=pltpu.VMEM)
HBM_SPEC = pl.BlockSpec(memory_space=pl.ANY)
FINISH_TILE = 256


def count_of(info_ref):
    return jnp.max(info_ref[info_ref.shape[0] - 8:, :]).astype(jnp.int32)


def live_tiles(info_ref):
    return (count_of(info_ref) + FINISH_TILE - 1) // FINISH_TILE


def prep_kernel(kappa, raw_hbm, q_hbm, count_ref, xv, rowv, info, forces, zeros, q_ref, sem, in_sems):
    rows = raw_hbm.shape[0]
    chunks = rows // CHUNK
    eye = lax.broadcasted_iota(jnp.int32, (CHUNK, CHUNK), 0) == lax.broadcasted_iota(jnp.int32, (CHUNK, CHUNK), 1)
    lane = lax.broadcasted_iota(jnp.int32, (1, CHUNK), 1)
    count = count_ref[0]
    group = rows // 4
    charge_copy = pltpu.make_async_copy(q_hbm, q_ref, in_sems.at[4])
    charge_copy.start()

    def fetch(g):
        return pltpu.make_async_copy(raw_hbm.at[pl.ds(g * group, group)], xv.at[pl.ds(g * group, group)], in_sems.at[g])

    for g in range(4):
        fetch(g).start()
    tiles = rows // FINISH_TILE
    live = (count + FINISH_TILE - 1) // FINISH_TILE
    zeros[...] = jnp.zeros_like(zeros)

    def blank(i):
        return pltpu.make_async_copy(zeros, forces.at[pl.ds(pl.multiple_of(i * FINISH_TILE, FINISH_TILE), FINISH_TILE)], sem)

    def start(i, _):
        blank(i).start()
        return 0

    lax.fori_loop(live, tiles, start, 0)
    info[2 * chunks:, :] = jnp.full((8, CHUNK), count, jnp.int32).astype(F32)

    def one(c, _):
        sl = pl.ds(pl.multiple_of(c * CHUNK, CHUNK), CHUNK)
        row_ids = lax.broadcasted_iota(jnp.int32, (CHUNK, 1), 0) + c * CHUNK
        block = jnp.where(row_ids < count, xv[sl, :].astype(F32), 0.0)
        xv[sl, :] = block.astype(xv.dtype)
        col_s = -kappa * jnp.sum(block * block, axis=1, keepdims=True)
        rowv[0, sl, :] = jnp.broadcast_to(col_s, (CHUNK, CHUNK))
        info[pl.ds(c, 1), :] = jnp.sum(jnp.where(eye, col_s, 0.0), axis=0, keepdims=True)
        live = jnp.where(lane + c * CHUNK < count, q_ref[pl.ds(c, 1), :], 0.0)
        info[pl.ds(chunks + c, 1), :] = live
        rowv[1, sl, :] = jnp.broadcast_to(jnp.sum(jnp.where(eye, live, 0.0), axis=1, keepdims=True), (CHUNK, CHUNK))
        return 0

    charge_copy.wait()
    for g in range(4):
        fetch(g).wait()
        lax.fori_loop(g * chunks // 4, (g + 1) * chunks // 4, one, 0)

    def wait(i, _):
        blank(i).wait()
        return 0

    lax.fori_loop(live, tiles, wait, 0)


def prep(x, charges, counts):
    rows, width = x.shape
    chunks = rows // CHUNK
    return pl.pallas_call(
        functools.partial(prep_kernel, LOG2E * 0.5 / width),
        out_shape=[jax.ShapeDtypeStruct(x.shape, x.dtype), pltpu.VMEM((2, rows, CHUNK), F32),
                   jax.ShapeDtypeStruct((2 * chunks + 8, CHUNK), F32), jax.ShapeDtypeStruct((rows, width), F32)],
        in_specs=[pl.BlockSpec(memory_space=pltpu.HBM)] * 2 + [pl.BlockSpec(memory_space=pltpu.SMEM)], out_specs=[VMEM_SPEC] * 3 + [HBM_SPEC],
        scratch_shapes=[pltpu.VMEM((FINISH_TILE, width), F32), pltpu.VMEM((chunks, CHUNK), F32), pltpu.SemaphoreType.DMA,
                        pltpu.SemaphoreType.DMA((5,))],
        compiler_params=pltpu.CompilerParams(vmem_limit_bytes=VMEM_LIMIT),
        name='prep')(x, charges.reshape(chunks, CHUNK), counts)


def weights(kappa, gram, row_a, row_c, col_a, col_c):
    expo = jnp.minimum(gram * (2.0 * kappa) + row_a + col_a, 0.0)
    return jnp.exp2(expo) * (row_c * col_c)


def step_kernel(cfg, *refs):
    start, num, tile_chunks, first, diag, kappa = cfg
    refs = list(refs)
    xv, rowv, my_info = refs[:3]
    refs = refs[3:]
    cols, src_info = xv, my_info
    if not diag:
        src_info, cols = refs[:2]
        refs = refs[2:]
    if not first:
        refs = refs[2:]
    tv, sv = refs[:2]
    rows, _ = xv.shape
    block_chunks = rows // CHUNK
    col_tile = tile_chunks * CHUNK
    live = jnp.clip((count_of(src_info) + CHUNK - 1) // CHUNK - start, 0, num)
    tiles = (live + tile_chunks - 1) // tile_chunks

    def old(ref, ct, rsl):
        return jnp.where(ct == 0, 0.0, ref[rsl, :]) if first else ref[rsl, :]

    def weigh(ct, c0, r0):
        rsl = pl.ds(r0, SUB_ROWS)
        s_sum = old(sv, ct, rsl)
        row_a = rowv[0, rsl, :]
        row_c = rowv[1, rsl, :]
        parts = []
        for q in range(tile_chunks // 2):
            gram = lax.dot_general(xv[rsl, :], cols[pl.ds(c0 + q * 256, 256), :], (((1,), (1,)), ((), ())),
                                   preferred_element_type=F32)
            for h in range(2):
                k = 2 * q + h
                cid = start + ct * tile_chunks + k
                col_a = src_info[pl.ds(cid, 1), :]
                col_c = src_info[pl.ds(block_chunks + cid, 1), :]
                w = weights(kappa, gram[:, h * 128:(h + 1) * 128], row_a, row_c, col_a, col_c)
                if diag:
                    delta = lax.broadcasted_iota(jnp.int32, w.shape, 0) - lax.broadcasted_iota(jnp.int32, w.shape, 1)
                    w = jnp.where(delta == c0 + k * CHUNK - r0, 0.0, w)
                s_sum = s_sum + w
                parts.append(w.astype(jnp.bfloat16))
        sv[rsl, :] = s_sum
        return jnp.concatenate(parts, axis=1)

    def pull(w, ct, c0, r0):
        rsl = pl.ds(r0, SUB_ROWS)
        tv[rsl, :] = old(tv, ct, rsl) + jnp.dot(w, cols[pl.ds(c0, col_tile), :], preferred_element_type=F32)

    def tile(ct, _):
        c0 = pl.multiple_of(ct * col_tile, col_tile)
        w = None
        for r0 in range(0, rows, SUB_ROWS):
            w_next = weigh(ct, c0, r0)
            if w is not None:
                pull(w, ct, c0, r0 - SUB_ROWS)
            w = w_next
        pull(w, ct, c0, rows - SUB_ROWS)
        return 0

    lax.fori_loop(0, tiles, tile, 0)


def last_kernel(cfg, xv, rowv, src_info, cols, s_in, sv, wv, part):
    start, num, kappa = cfg
    block_chunks = xv.shape[0] // CHUNK

    acc = jnp.zeros((8, 128), F32)
    for r0 in range(0, xv.shape[0], SUB_ROWS):
        rsl = pl.ds(r0, SUB_ROWS)
        gram = lax.dot_general(xv[rsl, :], cols[...], (((1,), (1,)), ((), ())), preferred_element_type=F32)
        sums = sv[rsl, :]
        for k in range(num):
            w = weights(kappa, gram[:, k * CHUNK:(k + 1) * CHUNK], rowv[0, rsl, :], rowv[1, rsl, :],
                        src_info[start + k:start + k + 1, :], src_info[block_chunks + start + k:block_chunks + start + k + 1, :])
            sums = sums + w
            wv[rsl, k * CHUNK:(k + 1) * CHUNK] = w.astype(jnp.bfloat16)
        sv[rsl, :] = sums
        for g in range(SUB_ROWS // 8):
            acc = acc + sums[g * 8:(g + 1) * 8]
    part[...] = acc


def last_step(x, rowf, src_info, cols, start, s_sum):
    rows, width = x.shape
    num = cols.shape[0] // CHUNK
    ins = [x, rowf, src_info, cols, s_sum]
    return pl.pallas_call(
        functools.partial(last_kernel, (start, num, LOG2E * 0.5 / width)),
        out_shape=[pltpu.VMEM((rows, 128), F32), pltpu.VMEM((rows, num * CHUNK), jnp.bfloat16), jax.ShapeDtypeStruct((8, 128), F32)],
        in_specs=[VMEM_SPEC] * len(ins), out_specs=[VMEM_SPEC] * 3,
        input_output_aliases={4: 0},
        compiler_params=pltpu.CompilerParams(vmem_limit_bytes=VMEM_LIMIT),
        cost_estimate=pl.CostEstimate(flops=2 * rows * num * CHUNK * width, bytes_accessed=rows * width, transcendentals=0),
        name='last')(*ins)


def finish_kernel(inv_len2, xv, tv, sv, wv, cols, my_info, blank, forces, buf, out_sems):
    del blank
    num = live_tiles(my_info)

    def out(i):
        return pltpu.make_async_copy(
            buf.at[lax.rem(i, 4)], forces.at[pl.ds(pl.multiple_of(i * FINISH_TILE, FINISH_TILE), FINISH_TILE)], out_sems.at[lax.rem(i, 4)])

    def one(i, _):
        @pl.when(i >= 4)
        def _():
            out(i - 4).wait()

        sl = pl.ds(pl.multiple_of(i * FINISH_TILE, FINISH_TILE), FINISH_TILE)
        total = jnp.sum(sv[sl, :], axis=1, keepdims=True)
        pulled = tv[sl, :] + jnp.dot(wv[sl, :], cols[...], preferred_element_type=F32)
        buf[lax.rem(i, 4)] = (total * xv[sl, :].astype(F32) - pulled) * inv_len2
        out(i).start()
        return 0

    lax.fori_loop(0, num, one, 0)

    def drain(i, _):
        out(i).wait()
        return 0

    lax.fori_loop(jnp.maximum(num - 4, 0), num, drain, 0)


def finish(*ins):
    x = ins[0]
    rows, width = x.shape
    return pl.pallas_call(
        functools.partial(finish_kernel, 1.0 / width),
        out_shape=jax.ShapeDtypeStruct((rows, width), F32),
        in_specs=[VMEM_SPEC] * (len(ins) - 1) + [HBM_SPEC], out_specs=HBM_SPEC,
        scratch_shapes=[pltpu.VMEM((4, FINISH_TILE, width), F32), pltpu.SemaphoreType.DMA((4,))],
        input_output_aliases={len(ins) - 1: 0},
        compiler_params=pltpu.CompilerParams(vmem_limit_bytes=VMEM_LIMIT),
        cost_estimate=pl.CostEstimate(flops=rows * width * 1000, bytes_accessed=rows * width * 4, transcendentals=0),
        name='finish')(*ins)


VMEM_LIMIT = 24 * 1024 * 1024


def step(x, rowf, my_info, src_info, cols, start, num, tile_chunks, carry):
    rows, width = x.shape
    first, diag = carry is None, cols is None
    cfg = (start, num, tile_chunks, first, diag, LOG2E * 0.5 / width)
    ins = [x, rowf, my_info] + ([] if diag else [src_info, cols]) + ([] if first else list(carry))
    in_specs = [VMEM_SPEC] * len(ins)
    flops = int(4 * rows * num * CHUNK * width * 0.6)
    common = dict(
        in_specs=in_specs,
        compiler_params=pltpu.CompilerParams(vmem_limit_bytes=VMEM_LIMIT),
        cost_estimate=pl.CostEstimate(flops=flops, bytes_accessed=rows * width, transcendentals=0),
        name='step_%d_%d' % (start, num))
    kernel = functools.partial(step_kernel, cfg)
    return pl.pallas_call(
        kernel,
        out_shape=[pltpu.VMEM((rows, width), F32), pltpu.VMEM((rows, 128), F32)],
        out_specs=[VMEM_SPEC] * 2,
        input_output_aliases={} if first else {len(ins) - 2: 0, len(ins) - 1: 1}, **common)(*ins)


PIECES = (256, 512, 512, 512, 256)


def solution(mesh):
    num_blocks = mesh.shape['row']
    cross_perm = [(src, src ^ 2) for src in range(num_blocks)]
    pair_perm = [(src, src ^ 1) for src in range(num_blocks)]
    diag_perm = [(src, src ^ 3) for src in range(num_blocks)]

    def per_device(positions, charges, counts):
        rows, _ = positions.shape
        chunks = rows // CHUNK
        head = jnp.where(jnp.arange(PIECES[0])[:, None] < counts[0], positions[:PIECES[0]], 0)
        arrived = [lax.ppermute(head, 'row', cross_perm)]
        x, rowf, info, blank = prep(positions, charges, counts)
        info_cross = lax.ppermute(info, 'row', cross_perm)
        info_pair = lax.ppermute(info, 'row', pair_perm)
        off = PIECES[0]
        for size in PIECES[1:]:
            arrived.append(lax.ppermute(x[off:off + size], 'row', cross_perm))
            off += size
        partner = lax.ppermute(x, 'row', pair_perm)
        carry = step(x, rowf, info, None, None, 0, chunks, 4, None)
        partner, *carry = lax.optimization_barrier((partner, *carry))
        carry = step(x, rowf, info, info_pair, partner, 0, chunks, 4, carry)
        info_cross, *carry = lax.optimization_barrier((info_cross, *carry))
        info_diag = lax.ppermute(info_cross, 'row', pair_perm)
        off = 0
        for k, piece in enumerate(arrived):
            num = PIECES[k] // CHUNK
            piece, *carry = lax.optimization_barrier((piece, *carry))
            relay = lax.ppermute(piece, 'row', pair_perm)
            carry = step(x, rowf, info, info_cross, piece, off, num, min(4, num), carry)
            if k < len(PIECES) - 1:
                carry = step(x, rowf, info, info_diag, relay, off, num, min(4, num), carry)
            else:
                t_sum, s_sum = carry
                s_sum, w_last, part = last_step(x, rowf, info_diag, relay, off, s_sum)
            off += num
        total = part
        for perm in (cross_perm, pair_perm, diag_perm):
            total = total + lax.ppermute(part, 'row', perm)
        forces = finish(x, t_sum, s_sum, w_last, relay, info, blank)
        return forces, (0.5 * jnp.sum(total)).reshape(1)

    row_spec = P(('sys', 'row'), None)
    vec_spec = P(('sys', 'row'))
    return jax.shard_map(per_device, mesh=mesh, in_specs=(row_spec, vec_spec, vec_spec), out_specs=(row_spec, P('sys')), check_vma=False)
```

```python
import functools

import jax
import jax.numpy as jnp
from jax import lax
from jax.experimental import pallas as pl
from jax.experimental.pallas import tpu as pltpu
from jax.sharding import PartitionSpec as P


CHUNK = 128
SUB_ROWS = 512
LOG2E = 1.4426950408889634
F32 = jnp.float32
VMEM_SPEC = pl.BlockSpec(memory_space=pltpu.VMEM)
HBM_SPEC = pl.BlockSpec(memory_space=pl.ANY)
FINISH_TILE = 256


def count_of(info_ref):
    return jnp.max(info_ref[info_ref.shape[0] - 8:, :]).astype(jnp.int32)


def prep_kernel(kappa, raw_hbm, q_hbm, count_ref, xv, rowv, info, forces, zeros, q_ref, sem, in_sems):
    rows = raw_hbm.shape[0]
    chunks = rows // CHUNK
    eye = lax.broadcasted_iota(jnp.int32, (CHUNK, CHUNK), 0) == lax.broadcasted_iota(jnp.int32, (CHUNK, CHUNK), 1)
    lane = lax.broadcasted_iota(jnp.int32, (1, CHUNK), 1)
    count = count_ref[0]
    group = rows // 4
    charge_copy = pltpu.make_async_copy(q_hbm, q_ref, in_sems.at[4])
    charge_copy.start()

    def fetch(g):
        return pltpu.make_async_copy(raw_hbm.at[pl.ds(g * group, group)], xv.at[pl.ds(g * group, group)], in_sems.at[g])

    for g in range(4):
        fetch(g).start()
    tiles = rows // FINISH_TILE
    live = (count + FINISH_TILE - 1) // FINISH_TILE
    zeros[...] = jnp.zeros_like(zeros)

    def blank(i):
        return pltpu.make_async_copy(zeros, forces.at[pl.ds(pl.multiple_of(i * FINISH_TILE, FINISH_TILE), FINISH_TILE)], sem)

    def start(i, _):
        blank(i).start()
        return 0

    lax.fori_loop(live, tiles, start, 0)
    info[2 * chunks:, :] = jnp.full((8, CHUNK), count, jnp.int32).astype(F32)

    def one(c, _):
        sl = pl.ds(pl.multiple_of(c * CHUNK, CHUNK), CHUNK)
        row_ids = lax.broadcasted_iota(jnp.int32, (CHUNK, 1), 0) + c * CHUNK
        block = jnp.where(row_ids < count, xv[sl, :].astype(F32), 0.0)
        xv[sl, :] = block.astype(xv.dtype)
        col_s = -kappa * jnp.sum(block * block, axis=1, keepdims=True)
        rowv[0, sl, :] = jnp.broadcast_to(col_s, (CHUNK, CHUNK))
        info[pl.ds(c, 1), :] = jnp.sum(jnp.where(eye, col_s, 0.0), axis=0, keepdims=True)
        live = jnp.where(lane + c * CHUNK < count, q_ref[pl.ds(c, 1), :], 0.0)
        info[pl.ds(chunks + c, 1), :] = live
        rowv[1, sl, :] = jnp.broadcast_to(jnp.sum(jnp.where(eye, live, 0.0), axis=1, keepdims=True), (CHUNK, CHUNK))
        return 0

    charge_copy.wait()
    for g in range(4):
        fetch(g).wait()
        lax.fori_loop(g * chunks // 4, (g + 1) * chunks // 4, one, 0)

    def wait(i, _):
        blank(i).wait()
        return 0

    lax.fori_loop(live, tiles, wait, 0)


def prep(x, charges, counts):
    rows, width = x.shape
    chunks = rows // CHUNK
    return pl.pallas_call(
        functools.partial(prep_kernel, LOG2E * 0.5 / width),
        out_shape=[jax.ShapeDtypeStruct(x.shape, x.dtype), pltpu.VMEM((2, rows, CHUNK), F32),
                   jax.ShapeDtypeStruct((2 * chunks + 8, CHUNK), F32), jax.ShapeDtypeStruct((rows, width), F32)],
        in_specs=[pl.BlockSpec(memory_space=pltpu.HBM)] * 2 + [pl.BlockSpec(memory_space=pltpu.SMEM)], out_specs=[VMEM_SPEC] * 3 + [HBM_SPEC],
        scratch_shapes=[pltpu.VMEM((FINISH_TILE, width), F32), pltpu.VMEM((chunks, CHUNK), F32), pltpu.SemaphoreType.DMA,
                        pltpu.SemaphoreType.DMA((5,))],
        compiler_params=pltpu.CompilerParams(vmem_limit_bytes=VMEM_LIMIT),
        name='prep')(x, charges.reshape(chunks, CHUNK), counts)


def weights(kappa, gram, row_a, row_c, col_a, col_c):
    expo = jnp.minimum(gram * (2.0 * kappa) + row_a + col_a, 0.0)
    return jnp.exp2(expo) * (row_c * col_c)


def step_kernel(cfg, *refs):
    start, num, tile_chunks, first, diag, kappa = cfg
    refs = list(refs)
    xv, rowv, my_info = refs[:3]
    refs = refs[3:]
    cols, src_info = xv, my_info
    if not diag:
        src_info, cols = refs[:2]
        refs = refs[2:]
    if not first:
        refs = refs[2:]
    tv, sv = refs[:2]
    rows, _ = xv.shape
    block_chunks = rows // CHUNK
    col_tile = tile_chunks * CHUNK
    live = jnp.clip((count_of(src_info) + CHUNK - 1) // CHUNK - start, 0, num)
    tiles = (live + tile_chunks - 1) // tile_chunks

    def old(ref, ct, rsl):
        return jnp.where(ct == 0, 0.0, ref[rsl, :]) if first else ref[rsl, :]

    def weigh(ct, c0, r0):
        rsl = pl.ds(r0, SUB_ROWS)
        s_sum = old(sv, ct, rsl)
        row_a = rowv[0, rsl, :]
        row_c = rowv[1, rsl, :]
        parts = []
        for q in range(tile_chunks // 2):
            gram = lax.dot_general(xv[rsl, :], cols[pl.ds(c0 + q * 256, 256), :], (((1,), (1,)), ((), ())),
                                   preferred_element_type=F32)
            for h in range(2):
                k = 2 * q + h
                cid = start + ct * tile_chunks + k
                col_a = src_info[pl.ds(cid, 1), :]
                col_c = src_info[pl.ds(block_chunks + cid, 1), :]
                w = weights(kappa, gram[:, h * 128:(h + 1) * 128], row_a, row_c, col_a, col_c)
                if diag:
                    delta = lax.broadcasted_iota(jnp.int32, w.shape, 0) - lax.broadcasted_iota(jnp.int32, w.shape, 1)
                    w = jnp.where(delta == c0 + k * CHUNK - r0, 0.0, w)
                s_sum = s_sum + w
                parts.append(w.astype(jnp.bfloat16))
        sv[rsl, :] = s_sum
        return jnp.concatenate(parts, axis=1)

    def pull(w, ct, c0, r0):
        rsl = pl.ds(r0, SUB_ROWS)
        tv[rsl, :] = old(tv, ct, rsl) + jnp.dot(w, cols[pl.ds(c0, col_tile), :], preferred_element_type=F32)

    def tile(ct, _):
        c0 = pl.multiple_of(ct * col_tile, col_tile)
        w = None
        for r0 in range(0, rows, SUB_ROWS):
            w_next = weigh(ct, c0, r0)
            if w is not None:
                pull(w, ct, c0, r0 - SUB_ROWS)
            w = w_next
        pull(w, ct, c0, rows - SUB_ROWS)
        return 0

    lax.fori_loop(0, tiles, tile, 0)


def last_kernel(cfg, xv, rowv, src_info, cols, s_in, sv, wv, part):
    start, num, kappa = cfg
    block_chunks = xv.shape[0] // CHUNK

    acc = jnp.zeros((8, 128), F32)
    for r0 in range(0, xv.shape[0], SUB_ROWS):
        rsl = pl.ds(r0, SUB_ROWS)
        gram = lax.dot_general(xv[rsl, :], cols[...], (((1,), (1,)), ((), ())), preferred_element_type=F32)
        sums = sv[rsl, :]
        for k in range(num):
            w = weights(kappa, gram[:, k * CHUNK:(k + 1) * CHUNK], rowv[0, rsl, :], rowv[1, rsl, :],
                        src_info[start + k:start + k + 1, :], src_info[block_chunks + start + k:block_chunks + start + k + 1, :])
            sums = sums + w
            wv[rsl, k * CHUNK:(k + 1) * CHUNK] = w.astype(jnp.bfloat16)
        sv[rsl, :] = sums
        for g in range(SUB_ROWS // 8):
            acc = acc + sums[g * 8:(g + 1) * 8]
    part[...] = acc


def last_step(x, rowf, src_info, cols, start, s_sum):
    rows, width = x.shape
    num = cols.shape[0] // CHUNK
    ins = [x, rowf, src_info, cols, s_sum]
    return pl.pallas_call(
        functools.partial(last_kernel, (start, num, LOG2E * 0.5 / width)),
        out_shape=[pltpu.VMEM((rows, 128), F32), pltpu.VMEM((rows, num * CHUNK), jnp.bfloat16), jax.ShapeDtypeStruct((8, 128), F32)],
        in_specs=[VMEM_SPEC] * len(ins), out_specs=[VMEM_SPEC] * 3,
        input_output_aliases={4: 0},
        compiler_params=pltpu.CompilerParams(vmem_limit_bytes=VMEM_LIMIT),
        cost_estimate=pl.CostEstimate(flops=2 * rows * num * CHUNK * width, bytes_accessed=rows * width, transcendentals=0),
        name='last')(*ins)


def finish_kernel(inv_len2, xv, tv, sv, wv, cols, count_ref, blank, forces, buf, out_sems):
    del blank
    num = (count_ref[0] + FINISH_TILE - 1) // FINISH_TILE

    def out(i):
        return pltpu.make_async_copy(
            buf.at[lax.rem(i, 4)], forces.at[pl.ds(pl.multiple_of(i * FINISH_TILE, FINISH_TILE), FINISH_TILE)], out_sems.at[lax.rem(i, 4)])

    def one(i, _):
        @pl.when(i >= 4)
        def _():
            out(i - 4).wait()

        sl = pl.ds(pl.multiple_of(i * FINISH_TILE, FINISH_TILE), FINISH_TILE)
        total = jnp.sum(sv[sl, :], axis=1, keepdims=True)
        pulled = tv[sl, :] + jnp.dot(wv[sl, :], cols[...], preferred_element_type=F32)
        buf[lax.rem(i, 4)] = (total * xv[sl, :].astype(F32) - pulled) * inv_len2
        out(i).start()
        return 0

    lax.fori_loop(0, num, one, 0)

    def drain(i, _):
        out(i).wait()
        return 0

    lax.fori_loop(jnp.maximum(num - 4, 0), num, drain, 0)


def finish(*ins):
    x = ins[0]
    rows, width = x.shape
    return pl.pallas_call(
        functools.partial(finish_kernel, 1.0 / width),
        out_shape=jax.ShapeDtypeStruct((rows, width), F32),
        in_specs=[VMEM_SPEC] * (len(ins) - 2) + [pl.BlockSpec(memory_space=pltpu.SMEM), HBM_SPEC], out_specs=HBM_SPEC,
        scratch_shapes=[pltpu.VMEM((4, FINISH_TILE, width), F32), pltpu.SemaphoreType.DMA((4,))],
        input_output_aliases={len(ins) - 1: 0},
        compiler_params=pltpu.CompilerParams(vmem_limit_bytes=VMEM_LIMIT),
        cost_estimate=pl.CostEstimate(flops=rows * width * 1000, bytes_accessed=rows * width * 4, transcendentals=0),
        name='finish')(*ins)


VMEM_LIMIT = 24 * 1024 * 1024


def step(x, rowf, my_info, src_info, cols, start, num, tile_chunks, carry):
    rows, width = x.shape
    first, diag = carry is None, cols is None
    cfg = (start, num, tile_chunks, first, diag, LOG2E * 0.5 / width)
    ins = [x, rowf, my_info] + ([] if diag else [src_info, cols]) + ([] if first else list(carry))
    in_specs = [VMEM_SPEC] * len(ins)
    flops = int(4 * rows * num * CHUNK * width * 0.6)
    common = dict(
        in_specs=in_specs,
        compiler_params=pltpu.CompilerParams(vmem_limit_bytes=VMEM_LIMIT),
        cost_estimate=pl.CostEstimate(flops=flops, bytes_accessed=rows * width, transcendentals=0),
        name='step_%d_%d' % (start, num))
    kernel = functools.partial(step_kernel, cfg)
    return pl.pallas_call(
        kernel,
        out_shape=[pltpu.VMEM((rows, width), F32), pltpu.VMEM((rows, 128), F32)],
        out_specs=[VMEM_SPEC] * 2,
        input_output_aliases={} if first else {len(ins) - 2: 0, len(ins) - 1: 1}, **common)(*ins)


PIECES = (512, 512, 512, 256, 256)


def solution(mesh):
    num_blocks = mesh.shape['row']
    cross_perm = [(src, src ^ 2) for src in range(num_blocks)]
    pair_perm = [(src, src ^ 1) for src in range(num_blocks)]
    diag_perm = [(src, src ^ 3) for src in range(num_blocks)]

    def per_device(positions, charges, counts):
        rows, _ = positions.shape
        chunks = rows // CHUNK
        head = jnp.where(jnp.arange(PIECES[0])[:, None] < counts[0], positions[:PIECES[0]], 0)
        arrived = [lax.ppermute(head, 'row', cross_perm)]
        x, rowf, info, blank = prep(positions, charges, counts)
        info_cross = lax.ppermute(info, 'row', cross_perm)
        info_pair = lax.ppermute(info, 'row', pair_perm)
        off = PIECES[0]
        for size in PIECES[1:]:
            arrived.append(lax.ppermute(x[off:off + size], 'row', cross_perm))
            off += size
        partner = lax.ppermute(x, 'row', pair_perm)
        carry = step(x, rowf, info, None, None, 0, chunks, 4, None)
        partner, *carry = lax.optimization_barrier((partner, *carry))
        carry = step(x, rowf, info, info_pair, partner, 0, chunks, 4, carry)
        info_cross, *carry = lax.optimization_barrier((info_cross, *carry))
        info_diag = lax.ppermute(info_cross, 'row', pair_perm)
        off = 0
        for k, piece in enumerate(arrived):
            num = PIECES[k] // CHUNK
            piece, *carry = lax.optimization_barrier((piece, *carry))
            relay = lax.ppermute(piece, 'row', pair_perm)
            carry = step(x, rowf, info, info_cross, piece, off, num, min(4, num), carry)
            if k < len(PIECES) - 1:
                carry = step(x, rowf, info, info_diag, relay, off, num, min(4, num), carry)
            else:
                t_sum, s_sum = carry
                s_sum, w_last, part = last_step(x, rowf, info_diag, relay, off, s_sum)
            off += num
        total = part
        for perm in (cross_perm, pair_perm, diag_perm):
            total = total + lax.ppermute(part, 'row', perm)
        forces = finish(x, t_sum, s_sum, w_last, relay, counts, blank)
        return forces, (0.5 * jnp.sum(total)).reshape(1)

    row_spec = P(('sys', 'row'), None)
    vec_spec = P(('sys', 'row'))
    return jax.shard_map(per_device, mesh=mesh, in_specs=(row_spec, vec_spec, vec_spec), out_specs=(row_spec, P('sys')), check_vma=False)
```
